32 devices in a mesh: pair: 2 (over x), seq: 8 (over z, y), head: 2 (over core).
Axes of the slice: x: 2, y: 2, z: 4, core: 2. Of those that a mesh axis runs over, the one named last changes fastest.
Arguments:
- queries: bfloat16 [2, 512, 2, 3584], P('pair', 'seq', None, 'head'), may hold values from -6 to 6
- answer_keys: bfloat16 [2, 512, 2, 512], P('pair', 'seq', None, 'head'), may hold values from -6 to 6
- answer_values: bfloat16 [2, 512, 2, 512], P('pair', 'seq', None, 'head'), may hold values from -6 to 6
- prefix_keys: bfloat16 [768, 512], P(('pair', 'seq'), 'head'), may hold values from -8 to 8
- prefix_values: bfloat16 [768, 512], P(('pair', 'seq'), 'head'), may hold values from -6 to 6
- grad_out: bfloat16 [2, 512, 2, 3584], P('pair', 'seq', None, 'head'), may hold values from -6 to 6
- answer_length: int32 [2, 2], P('pair'), may hold values from 128 to 512
- prefix_limit: int32 [2, 2], P('pair'), may hold values from 384 to 768
Outputs:
- attention_out: bfloat16 [2, 512, 2, 3584], P('pair', 'seq', None, 'head')
- grad_queries: bfloat16 [2, 512, 2, 3584], P('pair', 'seq', None, 'head')
- grad_answer_keys: bfloat16 [2, 512, 2, 512], P('pair', 'seq', None, 'head')
- grad_answer_values: bfloat16 [2, 512, 2, 512], P('pair', 'seq', None, 'head')
- grad_prefix_keys: float32 [768, 512], P(('pair', 'seq'), 'head')
- grad_prefix_values: float32 [768, 512], P(('pair', 'seq'), 'head')
The draws below stay inside these ranges and needn't reach their ends.
All inputs are finite; a program needn't handle non-finite values.
Results may differ from the reference program's by a relative error of at most 0.015.
Values may be sent and summed in bfloat16 or wider, within the bound.
No kernel may reach another device: no remote copies, remote signals or barrier semaphores. Data moves between devices by JAX's collectives and lax.ppermute only.
A program may use at most 64 MiB of HBM per device.

```python
from functools import partial
import jax
import jax.numpy as jnp
from jax import lax

HEADS = 28
KV_HEADS = 4
HEAD_DIM = 128
BATCH = 2
ANS = 512
PREFIX = 768


def draw_queries(key, part):
    shape = (2, ANS, BATCH, HEADS * HEAD_DIM)
    values = jax.random.normal(jax.random.fold_in(key, 11), shape, jnp.float32)
    return jnp.clip(values, -6.0, 6.0).astype(jnp.bfloat16)


def draw_prefix_keys(key, part):
    shape = (PREFIX, KV_HEADS * HEAD_DIM)
    values = jax.random.normal(jax.random.fold_in(key, 13), shape, jnp.float32)
    return jnp.clip(values, -6.0, 6.0).astype(jnp.bfloat16)


def plant(values, rng, smallest, high):
    longest = values.shape.index(max(values.shape))
    spots = []
    for shift in (0, 1):
        where = [jax.random.randint(jax.random.fold_in(rng, axis), (), 0, length) for axis, length in enumerate(values.shape)]
        where[longest] = (where[longest] + shift) % values.shape[longest]
        spots.append(tuple(where))
    return values.at[spots[0]].set(smallest).at[spots[1]].set(high)


def levels(own_key, dims, split, smallest, top_value):
    def one(position, blocks):
        heights = jax.random.uniform(jax.random.fold_in(jax.random.fold_in(own_key, 6), position), (blocks,), jnp.float32, smallest / len(split), top_value / len(split))
        return jnp.repeat(jnp.exp(heights), dims[position] // blocks).reshape((-1,) + (1,) * (len(dims) - position - 1))

    gain = one(*split[0])
    for cut in split[1:]:
        gain = gain * one(*cut)
    return gain


def gaussian(rng, dims, scale, limit, split=(), kind=jnp.bfloat16):
    values = jax.random.normal(rng, dims, jnp.float32) * scale
    if len(split) > 0:
        values = levels(rng, dims, split, -0.22, 0.18) * values
    return jnp.clip(values, min=-limit, max=limit).astype(kind)


def setup_inputs(seed: int = 0) -> dict:
    keys = jax.random.split(jax.random.key(seed), 9)
    return {
        "queries": draw_queries(jax.random.fold_in(keys[8], 71), 0),
        "answer_keys": gaussian(keys[1], (2, ANS, BATCH, KV_HEADS * HEAD_DIM), 1.0, 6.0, ((0, 2), (1, 8), (3, 2))),
        "answer_values": gaussian(keys[2], (2, ANS, BATCH, KV_HEADS * HEAD_DIM), 1.0, 6.0, ((0, 2), (1, 8), (3, 2))),
        "prefix_keys": draw_prefix_keys(jax.random.fold_in(keys[8], 71), 0),
        "prefix_values": gaussian(keys[4], (PREFIX, KV_HEADS * HEAD_DIM), 1.0, 6.0, ((0, 16), (1, 2))),
        "grad_out": gaussian(keys[5], (2, ANS, BATCH, HEADS * HEAD_DIM), 1.0, 6.0, ((0, 2), (1, 8), (3, 2))),
        "answer_length": plant(jax.random.randint(keys[6], (2, BATCH), ANS // 4, ANS + 1), jax.random.fold_in(keys[6], 1), ANS // 4, ANS).astype(jnp.int32),
        "prefix_limit": plant(jax.random.randint(keys[7], (2, BATCH), PREFIX // 2, PREFIX + 1), jax.random.fold_in(keys[7], 1), PREFIX // 2, PREFIX).astype(jnp.int32),
    }


negative_fill = -1e30


def one_head(pair_items, keys_all, values_all, limit_here, length):
    head_queries, head_douts = pair_items
    scaling = HEAD_DIM ** -0.5
    raw_scores = jnp.dot(head_queries, keys_all.T, preferred_element_type=jnp.float32) * scaling
    columns = jnp.arange(PREFIX + ANS, dtype=jnp.int32)[None, :]
    positions = jnp.arange(ANS, dtype=jnp.int32)[:, None]
    allowed = jnp.where(columns < PREFIX, columns < limit_here, columns - PREFIX <= positions)
    masked = jnp.where(allowed, raw_scores, negative_fill)
    top_score = jnp.max(masked, axis=1, keepdims=True)
    exp_total = jnp.sum(jnp.where(allowed, jnp.exp(masked - top_score), 0.0), axis=1, keepdims=True)
    log_total = top_score + jnp.log(exp_total)
    probs = jnp.where(allowed, jnp.exp(raw_scores - log_total), 0.0)
    probs_low = lax.optimization_barrier(probs.astype(jnp.bfloat16))
    live = positions < length
    attended = jnp.where(live, jnp.dot(probs_low, values_all, preferred_element_type=jnp.float32), 0.0)
    douts = jnp.where(live, head_douts, jnp.zeros_like(head_douts))
    grad_probs = jnp.dot(douts, values_all.T, preferred_element_type=jnp.float32)
    delta = jnp.sum(douts.astype(jnp.float32) * attended, axis=1, keepdims=True)
    grad_low = lax.optimization_barrier((probs * (grad_probs - delta)).astype(jnp.bfloat16))
    grad_queries = jnp.dot(grad_low, keys_all, preferred_element_type=jnp.float32) * scaling
    key_terms = jnp.dot(grad_low.T, head_queries, preferred_element_type=jnp.float32) * scaling
    value_terms = jnp.dot(probs_low.T, douts, preferred_element_type=jnp.float32)
    return attended.astype(jnp.bfloat16), grad_queries.astype(jnp.bfloat16), key_terms, value_terms


def reference(queries, answer_keys, answer_values, prefix_keys, prefix_values, grad_out, answer_length, prefix_limit):
    group_size = HEADS // KV_HEADS
    group_width = group_size * HEAD_DIM
    prefix_key_sums = [jnp.zeros((PREFIX, HEAD_DIM), jnp.float32) for head_index in range(KV_HEADS)]
    prefix_value_sums = [jnp.zeros((PREFIX, HEAD_DIM), jnp.float32) for head_index in range(KV_HEADS)]
    out_sides, query_sides, key_sides, value_sides = [], [], [], []
    for side_index in range(2):
        out_items, query_items, key_items, value_items = [], [], [], []
        for answer_index in range(BATCH):
            out_heads, query_heads, key_heads, value_heads = [], [], [], []
            for head_index in range(KV_HEADS):
                key_columns = slice(head_index * HEAD_DIM, (head_index + 1) * HEAD_DIM)
                query_columns = slice(head_index * group_width, (head_index + 1) * group_width)
                keys_all = jnp.concatenate([prefix_keys[:, key_columns], answer_keys[side_index, :, answer_index, key_columns]], axis=0)
                values_all = jnp.concatenate([prefix_values[:, key_columns], answer_values[side_index, :, answer_index, key_columns]], axis=0)
                head_queries = queries[side_index, :, answer_index, query_columns].reshape(ANS, group_size, HEAD_DIM).transpose(1, 0, 2)
                head_douts = grad_out[side_index, :, answer_index, query_columns].reshape(ANS, group_size, HEAD_DIM).transpose(1, 0, 2)
                results = lax.map(partial(one_head, keys_all=keys_all, values_all=values_all, limit_here=prefix_limit[side_index, answer_index], length=answer_length[side_index, answer_index]), (head_queries, head_douts))
                out_heads.append(results[0].transpose(1, 0, 2).reshape(ANS, group_width))
                query_heads.append(results[1].transpose(1, 0, 2).reshape(ANS, group_width))
                key_total = jnp.sum(results[2], axis=0)
                value_total = jnp.sum(results[3], axis=0)
                prefix_key_sums[head_index] = prefix_key_sums[head_index] + key_total[:PREFIX]
                prefix_value_sums[head_index] = prefix_value_sums[head_index] + value_total[:PREFIX]
                key_heads.append(key_total[PREFIX:].astype(jnp.bfloat16))
                value_heads.append(value_total[PREFIX:].astype(jnp.bfloat16))
            out_items.append(jnp.concatenate(out_heads, axis=1))
            query_items.append(jnp.concatenate(query_heads, axis=1))
            key_items.append(jnp.concatenate(key_heads, axis=1))
            value_items.append(jnp.concatenate(value_heads, axis=1))
        out_sides.append(jnp.stack(out_items, axis=1))
        query_sides.append(jnp.stack(query_items, axis=1))
        key_sides.append(jnp.stack(key_items, axis=1))
        value_sides.append(jnp.stack(value_items, axis=1))
    return (jnp.stack(out_sides), jnp.stack(query_sides), jnp.stack(key_sides), jnp.stack(value_sides), jnp.concatenate(prefix_key_sums, axis=1), jnp.concatenate(prefix_value_sums, axis=1))
```

```python
import math

import jax
import jax.numpy as jnp
from jax import lax
from jax.experimental import pallas as pl
from jax.experimental.pallas import tpu as pltpu
from jax.sharding import PartitionSpec as P

HEAD_DIM = 128
NEGATIVE = -1e30
LOG2E = math.log2(math.e)

f32 = jnp.float32
bf16 = jnp.bfloat16
CHUNK = 32


def mm(a, b):
    return jnp.dot(a, b, preferred_element_type=f32)


def mm_nt(a, b):
    return lax.dot_general(a, b, (((1,), (1,)), ((), ())), preferred_element_type=f32)


def mm_tn(a, b):
    return lax.dot_general(a, b, (((0,), (0,)), ((), ())), preferred_element_type=f32)


def params(cells):
    limit = 24 if cells <= 2**20 else 60
    return pltpu.CompilerParams(
        dimension_semantics=("arbitrary",), vmem_limit_bytes=limit * 1024 * 1024
    )


def cost(flops, moved, exps):
    return pl.CostEstimate(flops=flops, bytes_accessed=moved, transcendentals=exps)


def place_prefix(xy_ref, x_ref, k_s, v_s):
    rows = xy_ref.shape[-2]
    at = 0
    for ref in (xy_ref, x_ref):
        for yi in range(ref.shape[0]):
            for dz in range(ref.shape[1]):
                k_s[at : at + rows, :] = ref[yi, dz, 0, 0]
                v_s[at : at + rows, 0:HEAD_DIM] = ref[yi, dz, 1, 0]
                at += rows


def place_answer(refs, k_s, v_s):
    rows = refs[0].shape[-2]
    for t, ref in enumerate(refs):
        for b in range(ref.shape[2]):
            k_s[b, t * rows : (t + 1) * rows, :] = ref[0, 0, b]
            v_s[b, t * rows : (t + 1) * rows, 0:HEAD_DIM] = ref[1, 0, b]


def prefix_forward_body(
    bias_ref, q_ref, xy_ref, x_ref, p_ref, ol_ref, m_ref, k_s, v_s, s_s
):
    factor = HEAD_DIM ** (-0.5) * LOG2E
    batch = bias_ref.shape[0]
    total = q_ref.shape[1]
    per = total // batch
    place_prefix(xy_ref, x_ref, k_s, v_s)
    v_s[:, HEAD_DIM:] = jnp.ones((v_s.shape[0], HEAD_DIM), bf16)
    s_s[...] = mm_nt(q_ref[0], k_s[...])
    for b in range(batch):

        def step(i, carry, b=b):
            at = pl.multiple_of(b * per + i * CHUNK, CHUNK)
            s = s_s[pl.ds(at, CHUNK), :] + bias_ref[b, 0:1, :]
            top = jnp.max(s, axis=1, keepdims=True)
            p_ref[0, pl.ds(at, CHUNK), :] = jnp.exp2(s * factor - top * factor).astype(bf16)
            m_ref[0, pl.ds(at, CHUNK), :] = jnp.broadcast_to(top * factor, (CHUNK, HEAD_DIM))
            return carry

        lax.fori_loop(0, per // CHUNK, step, 0, unroll=2)
    ol_ref[0] = mm(p_ref[0], v_s[...])


def middle_body(
    pieces,
    live_ref,
    bias_ref,
    q_ref,
    do_ref,
    xy_ref,
    x_ref,
    p_ref,
    ol_ref,
    m_ref,
    *rest,
):
    answer = rest[:pieces]
    (
        out_ref,
        pb_ref,
        dob_ref,
        deltab_ref,
        dq_ref,
        own_ref,
        other_ref,
        k_s,
        v_s,
        s_s,
        ds_s,
        ka_s,
        va_s,
        olb_s,
        mb_s,
        doa_s,
        deltaa_s,
    ) = rest[pieces:]
    scale = HEAD_DIM ** (-0.5)
    factor = scale * LOG2E
    batch = ka_s.shape[0]
    keys = ka_s.shape[1]
    rows = bias_ref.shape[0]
    total = q_ref.shape[1]
    per = total // batch
    groups = per // rows
    place_answer(answer, ka_s, va_s)
    va_s[:, :, HEAD_DIM:] = jnp.ones((batch, keys, HEAD_DIM), bf16)
    place_prefix(xy_ref, x_ref, k_s, v_s)
    for b in range(batch):
        s_s[b * per : (b + 1) * per, 0:keys] = mm_nt(q_ref[0, b * per : (b + 1) * per, :], ka_s[b])
    halves = rows // CHUNK

    def soft(i, carry):
        for h in range(halves):
            at = pl.multiple_of(i * rows + h * CHUNK, CHUNK)
            s = s_s[pl.ds(at, CHUNK), 0:keys] + bias_ref[h * CHUNK : (h + 1) * CHUNK, :]
            top = jnp.max(s, axis=1, keepdims=True)
            pb_ref[0, pl.ds(at, CHUNK), :] = jnp.exp2(s * factor - top * factor).astype(bf16)
            mb_s[pl.ds(at, CHUNK), :] = jnp.broadcast_to(top * factor, (CHUNK, HEAD_DIM))
        return carry

    lax.fori_loop(0, batch * groups, soft, 0)
    for b in range(batch):
        olb_s[b * per : (b + 1) * per, :] = mm(pb_ref[0, b * per : (b + 1) * per, :], va_s[b])

    for b in range(batch):

        def combine(i, carry, b=b):
            at = pl.multiple_of(b * per + i * rows, rows)
            here = pl.ds(at, rows)
            live = live_ref[b]
            ma = m_ref[0, here, :]
            mb = mb_s[here, :]
            top = jnp.maximum(ma, mb)
            ea = jnp.exp2(ma - top)
            eb = jnp.exp2(mb - top)
            inverse = 1.0 / (
                ol_ref[0, here, HEAD_DIM:] * ea + olb_s[here, HEAD_DIM:] * eb
            )
            ea = ea * inverse
            eb = eb * inverse
            attended = (ol_ref[0, here, 0:HEAD_DIM] * ea + olb_s[here, 0:HEAD_DIM] * eb) * live
            out_ref[0, here, :] = attended.astype(bf16)
            douts = do_ref[0, here, :].astype(f32) * live
            da = (douts * ea).astype(bf16)
            db = (douts * eb).astype(bf16)
            doa_s[here, :] = da
            dob_ref[0, here, :] = db
            deltaa_s[here, :] = jnp.broadcast_to(
                jnp.sum(da.astype(f32) * attended, axis=1, keepdims=True), (rows, HEAD_DIM)
            )
            deltab_ref[0, here, :] = jnp.broadcast_to(
                jnp.sum(db.astype(f32) * attended, axis=1, keepdims=True), (rows, HEAD_DIM)
            )
            return carry

        lax.fori_loop(0, groups, combine, 0)
    s_s[...] = mm_nt(doa_s[...], v_s[...])

    def grad(i, carry):
        at = pl.multiple_of(i * CHUNK, CHUNK)
        here = pl.ds(at, CHUNK)
        ds_s[here, :] = (
            p_ref[0, here, :].astype(f32) * (s_s[here, :] - deltaa_s[here, 0:1])
        ).astype(bf16)
        return carry

    lax.fori_loop(0, total // CHUNK, grad, 0, unroll=2)
    dq_ref[0] = mm(ds_s[...], k_s[...])
    half = own_ref.shape[2]
    key_term = (jnp.transpose(mm_tn(q_ref[0], ds_s[...])) * scale).astype(bf16)
    own_ref[0, 0] = key_term[:half]
    other_ref[0, 0] = key_term[half:]
    value_term = jnp.transpose(mm_tn(doa_s[...], p_ref[0])).astype(bf16)
    own_ref[1, 0] = value_term[:half]
    other_ref[1, 0] = value_term[half:]


def answer_backward_body(pieces, q_ref, pb_ref, dob_ref, deltab_ref, dqa_ref, *rest):
    answer = rest[:pieces]
    dq_ref = rest[pieces]
    grads = rest[pieces + 1 : 2 * pieces + 1]
    ka_s, va_s, s_s, ds_s = rest[2 * pieces + 1 :]
    scale = HEAD_DIM ** (-0.5)
    batch = ka_s.shape[0]
    total = q_ref.shape[1]
    per = total // batch
    piece_rows = answer[0].shape[-2]
    place_answer(answer, ka_s, va_s)
    for b in range(batch):
        rows = slice(b * per, (b + 1) * per)
        s_s[rows, :] = mm_nt(dob_ref[0, rows, :], va_s[b])

    def grad(i, carry):
        at = pl.multiple_of(i * CHUNK, CHUNK)
        here = pl.ds(at, CHUNK)
        ds_s[here, :] = (
            pb_ref[0, here, :].astype(f32) * (s_s[here, :] - deltab_ref[0, here, 0:1])
        ).astype(bf16)
        return carry

    lax.fori_loop(0, total // CHUNK, grad, 0, unroll=2)
    for b in range(batch):
        rows = slice(b * per, (b + 1) * per)
        dq = dqa_ref[0, rows, :] + mm(ds_s[rows, :], ka_s[b])
        dq_ref[0, rows, :] = (dq * scale).astype(bf16)
        key_term = (jnp.transpose(mm_tn(q_ref[0, rows, :], ds_s[rows, :])) * scale).astype(bf16)
        value_term = jnp.transpose(mm_tn(dob_ref[0, rows, :], pb_ref[0, rows, :])).astype(bf16)
        for t, ref in enumerate(grads):
            span = slice(t * piece_rows, (t + 1) * piece_rows)
            ref[0, 0, b] = key_term[span]
            ref[1, 0, b] = value_term[span]


def on_device(
    queries,
    answer_keys,
    answer_values,
    prefix_keys,
    prefix_values,
    grad_out,
    answer_length,
    prefix_limit,
):
    size = lax.axis_size("seq")
    sides = lax.axis_size("pair")
    assert sides == 2 and size % 2 == 0
    outer = size // 2
    rows = queries.shape[1]
    batch = queries.shape[2]
    kv = answer_keys.shape[3] // HEAD_DIM
    group = queries.shape[3] // HEAD_DIM // kv
    per = group * rows
    total = batch * per
    prefix_rows = prefix_keys.shape[0]
    prefix_total = prefix_rows * size * sides
    answer_total = rows * size
    place = lax.axis_index("seq")
    side = lax.axis_index("pair")
    z, y = place // 2, place % 2

    def shift_z(x, k):
        return lax.ppermute(x, "seq", [(i, (i + 2 * k) % size) for i in range(size)])

    def swap_y(x):
        return lax.ppermute(x, "seq", [(i, i ^ 1) for i in range(size)])

    def swap_x(x):
        return lax.ppermute(x, "pair", [(0, 1), (1, 0)])

    prefix_own = jnp.stack(
        [a.reshape(prefix_rows, kv, HEAD_DIM).transpose(1, 0, 2) for a in (prefix_keys, prefix_values)]
    )
    answer_own = jnp.stack(
        [
            a[0].reshape(rows, batch, kv, HEAD_DIM).transpose(2, 1, 0, 3)
            for a in (answer_keys, answer_values)
        ]
    )
    prefix_z = jnp.stack([prefix_own] + [shift_z(prefix_own, k) for k in range(1, outer)])
    prefix_y = swap_y(prefix_z)
    prefix_here = jnp.stack([prefix_z, prefix_y])
    prefix_there = swap_x(prefix_here)
    near = [answer_own] + [shift_z(answer_own, k) for k in range(1, outer)]
    far = [swap_y(piece) for piece in near]
    answer = near + far
    pieces = len(answer)

    dz = jnp.arange(outer, dtype=jnp.int32)
    z_from = (z - dz) % outer
    pair_from = (side + jnp.arange(2, dtype=jnp.int32)) % 2
    y_from = (y + jnp.arange(2, dtype=jnp.int32)) % 2
    seq_from = z_from[None, :] * 2 + y_from[:, None]
    shard = pair_from[:, None, None] * size + seq_from[None]
    spots = (
        shard[..., None] * prefix_rows + jnp.arange(prefix_rows, dtype=jnp.int32)
    ).reshape(prefix_total)
    prefix_bias = jnp.where(spots[None, None, :] < prefix_limit[0][:, None, None], 0.0, NEGATIVE)
    prefix_bias = jnp.broadcast_to(prefix_bias, (batch, 8, prefix_total)).astype(f32)
    row_places = place * rows + jnp.arange(rows, dtype=jnp.int32)
    key_places = (
        seq_from[..., None] * rows + jnp.arange(rows, dtype=jnp.int32)
    ).reshape(answer_total)
    answer_bias = jnp.where(key_places[None, :] <= row_places[:, None], 0.0, NEGATIVE).astype(f32)
    live = jnp.where(row_places[None, :] < answer_length[0][:, None], 1.0, 0.0).astype(f32)
    live = jnp.broadcast_to(live[:, :, None], (batch, rows, HEAD_DIM))

    def head_major(x):
        x = x[0].reshape(rows, batch, kv, group, HEAD_DIM)
        return x.transpose(2, 1, 3, 0, 4).reshape(kv, total, HEAD_DIM)

    def row_major(x):
        x = x.reshape(kv, batch, group, rows, HEAD_DIM)
        return x.transpose(3, 1, 0, 2, 4).reshape(queries.shape)

    query_view = head_major(queries)
    grad_view = head_major(grad_out)

    def whole(shape):
        return pl.BlockSpec(shape, lambda c: (0,) * len(shape))

    def by_head(shape, axis=0):
        block = tuple(1 if a == axis else n for a, n in enumerate(shape))
        return pl.BlockSpec(block, lambda c: tuple(c if a == axis else 0 for a in range(len(shape))))

    q_shape = (kv, total, HEAD_DIM)
    q_spec = by_head(q_shape)
    prefix_spec = by_head(prefix_here.shape, 3)
    answer_spec = by_head(answer_own.shape, 1)
    pa_shape = (kv, total, prefix_total)
    pb_shape = (kv, total, answer_total)
    ol_shape = (kv, total, 2 * HEAD_DIM)
    grad_shape = (2, kv, prefix_total // 2, HEAD_DIM)
    grad_spec = by_head(grad_shape, 1)
    unit_a = 2 * kv * total * prefix_total * HEAD_DIM
    unit_b = 2 * kv * total * answer_total * HEAD_DIM

    probs_a, ol_a, top_a = pl.pallas_call(
        prefix_forward_body,
        grid=(kv,),
        in_specs=[whole(prefix_bias.shape), q_spec, prefix_spec, prefix_spec],
        out_specs=[by_head(pa_shape), by_head(ol_shape), q_spec],
        out_shape=[
            jax.ShapeDtypeStruct(pa_shape, bf16),
            jax.ShapeDtypeStruct(ol_shape, f32),
            jax.ShapeDtypeStruct(q_shape, f32),
        ],
        scratch_shapes=[
            pltpu.VMEM((prefix_total, HEAD_DIM), bf16),
            pltpu.VMEM((prefix_total, 2 * HEAD_DIM), bf16),
            pltpu.VMEM((total, prefix_total), f32),
        ],
        compiler_params=params(total * prefix_total),
        cost_estimate=cost(2 * unit_a, 8 << 20, kv * total * prefix_total),
        name="prefix_forward",
    )(prefix_bias, query_view, prefix_here, prefix_there)

    out_view, probs_b, grad_b, delta_b, dq_a, prefix_own_sum, prefix_other_sum = pl.pallas_call(
        lambda *refs: middle_body(pieces, *refs),
        grid=(kv,),
        in_specs=[
            whole(live.shape),
            whole(answer_bias.shape),
            q_spec,
            q_spec,
            prefix_spec,
            prefix_spec,
            by_head(pa_shape),
            by_head(ol_shape),
            q_spec,
        ]
        + [answer_spec] * pieces,
        out_specs=[q_spec, by_head(pb_shape), q_spec, q_spec, q_spec, grad_spec, grad_spec],
        out_shape=[
            jax.ShapeDtypeStruct(q_shape, bf16),
            jax.ShapeDtypeStruct(pb_shape, bf16),
            jax.ShapeDtypeStruct(q_shape, bf16),
            jax.ShapeDtypeStruct(q_shape, f32),
            jax.ShapeDtypeStruct(q_shape, f32),
            jax.ShapeDtypeStruct(grad_shape, bf16),
            jax.ShapeDtypeStruct(grad_shape, bf16),
        ],
        scratch_shapes=[
            pltpu.VMEM((prefix_total, HEAD_DIM), bf16),
            pltpu.VMEM((prefix_total, HEAD_DIM), bf16),
            pltpu.VMEM((total, max(prefix_total, answer_total)), f32),
            pltpu.VMEM((total, prefix_total), bf16),
            pltpu.VMEM((batch, answer_total, HEAD_DIM), bf16),
            pltpu.VMEM((batch, answer_total, 2 * HEAD_DIM), bf16),
            pltpu.VMEM((total, 2 * HEAD_DIM), f32),
            pltpu.VMEM((total, HEAD_DIM), f32),
            pltpu.VMEM((total, HEAD_DIM), bf16),
            pltpu.VMEM((total, HEAD_DIM), f32),
        ],
        compiler_params=params(total * prefix_total),
        cost_estimate=cost(2 * unit_b + 4 * unit_a, 12 << 20, kv * total * answer_total),
        name="middle",
    )(
        live,
        answer_bias,
        query_view,
        grad_view,
        prefix_here,
        prefix_there,
        probs_a,
        ol_a,
        top_a,
        *answer,
    )

    dq_view, *answer_grads = pl.pallas_call(
        lambda *refs: answer_backward_body(pieces, *refs),
        grid=(kv,),
        in_specs=[q_spec, by_head(pb_shape), q_spec, q_spec, q_spec] + [answer_spec] * pieces,
        out_specs=[q_spec] + [answer_spec] * pieces,
        out_shape=[jax.ShapeDtypeStruct(q_shape, bf16)]
        + [jax.ShapeDtypeStruct(answer_own.shape, bf16)] * pieces,
        scratch_shapes=[
            pltpu.VMEM((batch, answer_total, HEAD_DIM), bf16),
            pltpu.VMEM((batch, answer_total, HEAD_DIM), bf16),
            pltpu.VMEM((total, answer_total), f32),
            pltpu.VMEM((total, answer_total), bf16),
        ],
        compiler_params=params(total * prefix_total),
        cost_estimate=cost(4 * unit_b, 8 << 20, 0),
        name="answer_backward",
    )(query_view, probs_b, grad_b, delta_b, dq_a, *answer)

    split = (2, kv, 2, outer, prefix_rows, HEAD_DIM)
    x_got = swap_x(prefix_other_sum).reshape(split).astype(f32)
    x_own = prefix_own_sum.reshape(split).astype(f32)
    y_got = swap_y((x_own[:, :, 1] + x_got[:, :, 1]).astype(bf16)).astype(f32)
    z_sum = x_own[:, :, 0] + x_got[:, :, 0] + y_got
    prefix_sum = z_sum[:, :, 0]
    for k in range(1, outer):
        prefix_sum = prefix_sum + shift_z(z_sum[:, :, k].astype(bf16), -k).astype(f32)
    answer_sum = None
    for k in reversed(range(outer)):
        piece = answer_grads[k].astype(f32) + swap_y(answer_grads[outer + k]).astype(f32)
        if k:
            piece = shift_z(piece.astype(bf16), -k).astype(f32)
        answer_sum = piece if answer_sum is None else answer_sum + piece
    answer_sum = answer_sum.astype(bf16)

    def prefix_out(x):
        return x.transpose(1, 0, 2).reshape(prefix_keys.shape)

    def answer_out(x):
        return x.transpose(2, 1, 0, 3).reshape(answer_keys.shape)

    return (
        row_major(out_view),
        row_major(dq_view),
        answer_out(answer_sum[0]),
        answer_out(answer_sum[1]),
        prefix_out(prefix_sum[0]),
        prefix_out(prefix_sum[1]),
    )


def solution(mesh):
    wide = P("pair", "seq", None, "head")
    shared = P(("pair", "seq"), "head")
    small = P("pair", None)
    return jax.shard_map(
        on_device,
        mesh=mesh,
        in_specs=(wide, wide, wide, shared, shared, wide, small, small),
        out_specs=(wide, wide, wide, wide, shared, shared),
        check_vma=False,
    )
```

```python
import math

import jax
import jax.numpy as jnp
from jax import lax
from jax.experimental import pallas as pl
from jax.experimental.pallas import tpu as pltpu
from jax.sharding import PartitionSpec as P

HEAD_DIM = 128
NEGATIVE = -1e30
LOG2E = math.log2(math.e)

f32 = jnp.float32
bf16 = jnp.bfloat16
CHUNK = 32


def mm(a, b):
    return jnp.dot(a, b, preferred_element_type=f32)


def mm_nt(a, b):
    return lax.dot_general(a, b, (((1,), (1,)), ((), ())), preferred_element_type=f32)


def mm_tn(a, b):
    return lax.dot_general(a, b, (((0,), (0,)), ((), ())), preferred_element_type=f32)


def params(cells):
    limit = 24 if cells <= 2**20 else 60
    return pltpu.CompilerParams(
        dimension_semantics=("arbitrary",), vmem_limit_bytes=limit * 1024 * 1024
    )


def cost(flops, moved, exps):
    return pl.CostEstimate(flops=flops, bytes_accessed=moved, transcendentals=exps)


def place_prefix(xy_ref, x_ref, k_s, v_s):
    rows = xy_ref.shape[-2]
    at = 0
    for ref in (xy_ref, x_ref):
        for yi in range(ref.shape[0]):
            for dz in range(ref.shape[1]):
                k_s[at : at + rows, :] = ref[yi, dz, 0, 0]
                if v_s is not None:
                    v_s[at : at + rows, 0:HEAD_DIM] = ref[yi, dz, 1, 0]
                at += rows


def place_answer(refs, k_s, v_s):
    rows = refs[0].shape[-2]
    for t, ref in enumerate(refs):
        for b in range(ref.shape[2]):
            k_s[b, t * rows : (t + 1) * rows, :] = ref[0, 0, b]
            v_s[b, t * rows : (t + 1) * rows, 0:HEAD_DIM] = ref[1, 0, b]


def lanes(ref, here, update):
    for j in range(ref.shape[-1] // HEAD_DIM):
        columns = slice(j * HEAD_DIM, (j + 1) * HEAD_DIM)
        ref[0, here, columns] = update(columns)


def exponents(p_ref, s_s, m_s, first, rows):
    factor = HEAD_DIM ** (-0.5) * LOG2E

    def step(i, carry):
        here = pl.ds(pl.multiple_of(first + i * CHUNK, CHUNK), CHUNK)
        top = m_s(here)
        lanes(p_ref, here, lambda c: jnp.exp2(s_s[here, c] * factor - top).astype(bf16))
        return carry

    lax.fori_loop(0, rows // CHUNK, step, 0, unroll=7)


def blocks(total, rows, columns):
    size = total if total * columns <= 2**19 else rows
    return [slice(a, a + size) for a in range(0, total, size)]


def row_top(s):
    factor = HEAD_DIM ** (-0.5) * LOG2E
    top = jnp.max(s, axis=1, keepdims=True) * factor
    return jnp.broadcast_to(top, (s.shape[0], HEAD_DIM))


def score_grads(ds_s, p, dp, delta):
    for j in range(ds_s.shape[-1] // HEAD_DIM):
        columns = slice(j * HEAD_DIM, (j + 1) * HEAD_DIM)
        ds_s[:, columns] = (p[:, columns].astype(f32) * (dp[:, columns] - delta)).astype(bf16)


def prefix_forward_body(
    bias_ref, q_ref, xy_ref, x_ref, p_ref, ol_ref, m_ref, k_s, v_s, s_s
):
    batch = bias_ref.shape[0]
    total = q_ref.shape[1]
    per = total // batch
    place_prefix(xy_ref, x_ref, k_s, v_s)
    v_s[:, HEAD_DIM:] = jnp.ones((v_s.shape[0], HEAD_DIM), bf16)
    for b in range(batch):
        for part in blocks(per, 64, k_s.shape[0]):
            rows = slice(b * per + part.start, b * per + part.stop)
            s = mm_nt(q_ref[0, rows, :], k_s[...]) + bias_ref[b, 0:1, :]
            s_s[rows, :] = s
            m_ref[0, rows, :] = row_top(s)
    for b in range(batch):
        rows = slice(b * per, (b + 1) * per)
        exponents(p_ref, s_s, lambda here: m_ref[0, here, :], b * per, per)
        ol_ref[0, rows, :] = mm(p_ref[0, rows, :], v_s[...])


def middle_body(
    pieces,
    live_ref,
    bias_ref,
    q_ref,
    do_ref,
    xy_ref,
    x_ref,
    p_ref,
    ol_ref,
    m_ref,
    *rest,
):
    answer = rest[:pieces]
    (
        out_ref,
        pb_ref,
        dob_ref,
        deltab_ref,
        ds_ref,
        own_ref,
        other_ref,
        k_s,
        v_s,
        s_s,
        ka_s,
        va_s,
        olb_s,
        mb_s,
        doa_s,
        deltaa_s,
    ) = rest[pieces:]
    scale = HEAD_DIM ** (-0.5)
    batch = ka_s.shape[0]
    keys = ka_s.shape[1]
    rows = bias_ref.shape[0]
    total = q_ref.shape[1]
    per = total // batch
    groups = per // rows
    place_answer(answer, ka_s, va_s)
    va_s[:, :, HEAD_DIM:] = jnp.ones((batch, keys, HEAD_DIM), bf16)
    place_prefix(xy_ref, x_ref, k_s, v_s)
    for b in range(batch):
        for part in blocks(per, rows, keys):
            base = b * per + part.start
            size = part.stop - part.start
            scores = mm_nt(q_ref[0, base : base + size, :], ka_s[b])
            for g in range(size // rows):
                span = slice(base + g * rows, base + (g + 1) * rows)
                s = scores[g * rows : (g + 1) * rows, :] + bias_ref[...]
                s_s[span, :] = s
                mb_s[span, :] = row_top(s)
    for b in range(batch):
        exponents(pb_ref, s_s, lambda here: mb_s[here, :], b * per, per)
        olb_s[b * per : (b + 1) * per, :] = mm(pb_ref[0, b * per : (b + 1) * per, :], va_s[b])

    for b in range(batch):

        def combine(i, carry, b=b):
            here = pl.ds(pl.multiple_of(b * per + i * rows, rows), rows)
            live = live_ref[b]
            ma = m_ref[0, here, :]
            mb = mb_s[here, :]
            top = jnp.maximum(ma, mb)
            ea = jnp.exp2(ma - top)
            eb = jnp.exp2(mb - top)
            inverse = 1.0 / (
                ol_ref[0, here, HEAD_DIM:] * ea + olb_s[here, HEAD_DIM:] * eb
            )
            ea = ea * inverse
            eb = eb * inverse
            attended = (ol_ref[0, here, 0:HEAD_DIM] * ea + olb_s[here, 0:HEAD_DIM] * eb) * live
            out_ref[0, here, :] = attended.astype(bf16)
            douts = do_ref[0, here, :].astype(f32) * live
            da = (douts * ea).astype(bf16)
            db = (douts * eb).astype(bf16)
            doa_s[here, :] = da
            dob_ref[0, here, :] = db
            deltaa_s[here, :] = jnp.broadcast_to(
                jnp.sum(da.astype(f32) * attended, axis=1, keepdims=True), (rows, HEAD_DIM)
            )
            deltab_ref[0, here, :] = jnp.broadcast_to(
                jnp.sum(db.astype(f32) * attended, axis=1, keepdims=True), (rows, HEAD_DIM)
            )
            return carry

        lax.fori_loop(0, groups, combine, 0, unroll=groups)
    for span in blocks(total, per if per * k_s.shape[0] <= 2**19 else rows, k_s.shape[0]):
        dp = mm_nt(doa_s[span, :], v_s[...])
        score_grads(ds_ref.at[0, span], p_ref[0, span, :], dp, deltaa_s[span, :])
    half = own_ref.shape[2]
    value_term = jnp.transpose(mm_tn(doa_s[...], p_ref[0])).astype(bf16)
    own_ref[1, 0] = value_term[:half]
    other_ref[1, 0] = value_term[half:]
    key_term = (jnp.transpose(mm_tn(q_ref[0], ds_ref[0])) * scale).astype(bf16)
    own_ref[0, 0] = key_term[:half]
    other_ref[0, 0] = key_term[half:]


def answer_backward_body(
    pieces, q_ref, xy_ref, x_ref, ds_ref, pb_ref, dob_ref, deltab_ref, *rest
):
    answer = rest[:pieces]
    dq_ref = rest[pieces]
    grads = rest[pieces + 1 : 2 * pieces + 1]
    k_s, ka_s, va_s, dsb_s = rest[2 * pieces + 1 :]
    scale = HEAD_DIM ** (-0.5)
    batch = ka_s.shape[0]
    total = q_ref.shape[1]
    per = total // batch
    piece_rows = answer[0].shape[-2]
    place_answer(answer, ka_s, va_s)
    place_prefix(xy_ref, x_ref, k_s, None)
    for b in range(batch):
        for part in blocks(per, 64, ka_s.shape[1]):
            rows = slice(b * per + part.start, b * per + part.stop)
            dp = mm_nt(dob_ref[0, rows, :], va_s[b])
            score_grads(dsb_s.at[rows], pb_ref[0, rows, :], dp, deltab_ref[0, rows, :])
    for b in range(batch):
        rows = slice(b * per, (b + 1) * per)
        key_term = (jnp.transpose(mm_tn(q_ref[0, rows, :], dsb_s[rows, :])) * scale).astype(bf16)
        value_term = jnp.transpose(mm_tn(dob_ref[0, rows, :], pb_ref[0, rows, :])).astype(bf16)
        for t, ref in enumerate(grads):
            span = slice(t * piece_rows, (t + 1) * piece_rows)
            ref[0, 0, b] = key_term[span]
            ref[1, 0, b] = value_term[span]
    for b in range(batch):
        rows = slice(b * per, (b + 1) * per)
        dq = mm(ds_ref[0, rows, :], k_s[...]) + mm(dsb_s[rows, :], ka_s[b])
        dq_ref[0, rows, :] = (dq * scale).astype(bf16)


def on_device(
    queries,
    answer_keys,
    answer_values,
    prefix_keys,
    prefix_values,
    grad_out,
    answer_length,
    prefix_limit,
):
    size = lax.axis_size("seq")
    sides = lax.axis_size("pair")
    assert sides == 2 and size % 2 == 0
    outer = size // 2
    rows = queries.shape[1]
    batch = queries.shape[2]
    kv = answer_keys.shape[3] // HEAD_DIM
    group = queries.shape[3] // HEAD_DIM // kv
    per = group * rows
    total = batch * per
    prefix_rows = prefix_keys.shape[0]
    prefix_total = prefix_rows * size * sides
    answer_total = rows * size
    place = lax.axis_index("seq")
    side = lax.axis_index("pair")
    z, y = place // 2, place % 2

    def shift_z(x, k):
        return lax.ppermute(x, "seq", [(i, (i + 2 * k) % size) for i in range(size)])

    def swap_y(x):
        return lax.ppermute(x, "seq", [(i, i ^ 1) for i in range(size)])

    def swap_x(x):
        return lax.ppermute(x, "pair", [(0, 1), (1, 0)])

    prefix_own = jnp.stack(
        [a.reshape(prefix_rows, kv, HEAD_DIM).transpose(1, 0, 2) for a in (prefix_keys, prefix_values)]
    )
    answer_own = jnp.stack(
        [
            a[0].reshape(rows, batch, kv, HEAD_DIM).transpose(2, 1, 0, 3)
            for a in (answer_keys, answer_values)
        ]
    )
    prefix_z = jnp.stack([prefix_own] + [shift_z(prefix_own, k) for k in range(1, outer)])
    prefix_y = swap_y(prefix_z)
    prefix_here = jnp.stack([prefix_z, prefix_y])
    prefix_there = swap_x(prefix_here)
    near = [answer_own] + [shift_z(answer_own, k) for k in range(1, outer)]
    far = [swap_y(piece) for piece in near]
    answer = near + far
    pieces = len(answer)

    dz = jnp.arange(outer, dtype=jnp.int32)
    z_from = (z - dz) % outer
    pair_from = (side + jnp.arange(2, dtype=jnp.int32)) % 2
    y_from = (y + jnp.arange(2, dtype=jnp.int32)) % 2
    seq_from = z_from[None, :] * 2 + y_from[:, None]
    shard = pair_from[:, None, None] * size + seq_from[None]
    spots = (
        shard[..., None] * prefix_rows + jnp.arange(prefix_rows, dtype=jnp.int32)
    ).reshape(prefix_total)
    prefix_bias = jnp.where(spots[None, None, :] < prefix_limit[0][:, None, None], 0.0, NEGATIVE)
    prefix_bias = jnp.broadcast_to(prefix_bias, (batch, 8, prefix_total)).astype(f32)
    row_places = place * rows + jnp.arange(rows, dtype=jnp.int32)
    key_places = (
        seq_from[..., None] * rows + jnp.arange(rows, dtype=jnp.int32)
    ).reshape(answer_total)
    answer_bias = jnp.where(key_places[None, :] <= row_places[:, None], 0.0, NEGATIVE).astype(f32)
    live = jnp.where(row_places[None, :] < answer_length[0][:, None], 1.0, 0.0).astype(f32)
    live = jnp.broadcast_to(live[:, :, None], (batch, rows, HEAD_DIM))

    def head_major(x):
        x = x[0].reshape(rows, batch, kv, group, HEAD_DIM)
        return x.transpose(2, 1, 3, 0, 4).reshape(kv, total, HEAD_DIM)

    def row_major(x):
        x = x.reshape(kv, batch, group, rows, HEAD_DIM)
        return x.transpose(3, 1, 0, 2, 4).reshape(queries.shape)

    query_view = head_major(queries)
    grad_view = head_major(grad_out)

    def whole(shape):
        return pl.BlockSpec(shape, lambda c: (0,) * len(shape))

    def by_head(shape, axis=0):
        block = tuple(1 if a == axis else n for a, n in enumerate(shape))
        return pl.BlockSpec(block, lambda c: tuple(c if a == axis else 0 for a in range(len(shape))))

    q_shape = (kv, total, HEAD_DIM)
    q_spec = by_head(q_shape)
    prefix_spec = by_head(prefix_here.shape, 3)
    answer_spec = by_head(answer_own.shape, 1)
    pa_shape = (kv, total, prefix_total)
    pb_shape = (kv, total, answer_total)
    ol_shape = (kv, total, 2 * HEAD_DIM)
    grad_shape = (2, kv, prefix_total // 2, HEAD_DIM)
    grad_spec = by_head(grad_shape, 1)
    unit_a = 2 * kv * total * prefix_total * HEAD_DIM
    unit_b = 2 * kv * total * answer_total * HEAD_DIM

    probs_a, ol_a, top_a = pl.pallas_call(
        prefix_forward_body,
        grid=(kv,),
        in_specs=[whole(prefix_bias.shape), q_spec, prefix_spec, prefix_spec],
        out_specs=[by_head(pa_shape), by_head(ol_shape), q_spec],
        out_shape=[
            jax.ShapeDtypeStruct(pa_shape, bf16),
            jax.ShapeDtypeStruct(ol_shape, f32),
            jax.ShapeDtypeStruct(q_shape, f32),
        ],
        scratch_shapes=[
            pltpu.VMEM((prefix_total, HEAD_DIM), bf16),
            pltpu.VMEM((prefix_total, 2 * HEAD_DIM), bf16),
            pltpu.VMEM((total, prefix_total), f32),
        ],
        compiler_params=params(total * prefix_total),
        cost_estimate=cost(2 * unit_a, 8 << 20, kv * total * prefix_total),
        name="prefix_forward",
    )(prefix_bias, query_view, prefix_here, prefix_there)

    out_view, probs_b, grad_b, delta_b, ds_a, prefix_own_sum, prefix_other_sum = pl.pallas_call(
        lambda *refs: middle_body(pieces, *refs),
        grid=(kv,),
        in_specs=[
            whole(live.shape),
            whole(answer_bias.shape),
            q_spec,
            q_spec,
            prefix_spec,
            prefix_spec,
            by_head(pa_shape),
            by_head(ol_shape),
            q_spec,
        ]
        + [answer_spec] * pieces,
        out_specs=[
            q_spec, by_head(pb_shape), q_spec, q_spec, by_head(pa_shape), grad_spec, grad_spec
        ],
        out_shape=[
            jax.ShapeDtypeStruct(q_shape, bf16),
            jax.ShapeDtypeStruct(pb_shape, bf16),
            jax.ShapeDtypeStruct(q_shape, bf16),
            jax.ShapeDtypeStruct(q_shape, f32),
            jax.ShapeDtypeStruct(pa_shape, bf16),
            jax.ShapeDtypeStruct(grad_shape, bf16),
            jax.ShapeDtypeStruct(grad_shape, bf16),
        ],
        scratch_shapes=[
            pltpu.VMEM((prefix_total, HEAD_DIM), bf16),
            pltpu.VMEM((prefix_total, HEAD_DIM), bf16),
            pltpu.VMEM((total, answer_total), f32),
            pltpu.VMEM((batch, answer_total, HEAD_DIM), bf16),
            pltpu.VMEM((batch, answer_total, 2 * HEAD_DIM), bf16),
            pltpu.VMEM((total, 2 * HEAD_DIM), f32),
            pltpu.VMEM((total, HEAD_DIM), f32),
            pltpu.VMEM((total, HEAD_DIM), bf16),
            pltpu.VMEM((total, HEAD_DIM), f32),
        ],
        compiler_params=params(total * prefix_total),
        cost_estimate=cost(2 * unit_b + 3 * unit_a, 12 << 20, kv * total * answer_total),
        name="middle",
    )(
        live,
        answer_bias,
        query_view,
        grad_view,
        prefix_here,
        prefix_there,
        probs_a,
        ol_a,
        top_a,
        *answer,
    )

    dq_view, *answer_grads = pl.pallas_call(
        lambda *refs: answer_backward_body(pieces, *refs),
        grid=(kv,),
        in_specs=[
            q_spec,
            prefix_spec,
            prefix_spec,
            by_head(pa_shape),
            by_head(pb_shape),
            q_spec,
            q_spec,
        ]
        + [answer_spec] * pieces,
        out_specs=[q_spec] + [answer_spec] * pieces,
        out_shape=[jax.ShapeDtypeStruct(q_shape, bf16)]
        + [jax.ShapeDtypeStruct(answer_own.shape, bf16)] * pieces,
        scratch_shapes=[
            pltpu.VMEM((prefix_total, HEAD_DIM), bf16),
            pltpu.VMEM((batch, answer_total, HEAD_DIM), bf16),
            pltpu.VMEM((batch, answer_total, HEAD_DIM), bf16),
            pltpu.VMEM((total, answer_total), bf16),
        ],
        compiler_params=params(total * prefix_total),
        cost_estimate=cost(4 * unit_b + unit_a, 8 << 20, 0),
        name="answer_backward",
    )(
        query_view, prefix_here, prefix_there, ds_a, probs_b, grad_b, delta_b, *answer
    )

    split = (2, kv, 2, outer, prefix_rows, HEAD_DIM)
    x_got = swap_x(prefix_other_sum).reshape(split).astype(f32)
    x_own = prefix_own_sum.reshape(split).astype(f32)
    y_got = swap_y((x_own[:, :, 1] + x_got[:, :, 1]).astype(bf16)).astype(f32)
    z_sum = x_own[:, :, 0] + x_got[:, :, 0] + y_got
    prefix_sum = z_sum[:, :, 0]
    for k in range(1, outer):
        prefix_sum = prefix_sum + shift_z(z_sum[:, :, k].astype(bf16), -k).astype(f32)
    answer_sum = None
    for k in reversed(range(outer)):
        piece = answer_grads[k].astype(f32) + swap_y(answer_grads[outer + k]).astype(f32)
        if k:
            piece = shift_z(piece.astype(bf16), -k).astype(f32)
        answer_sum = piece if answer_sum is None else answer_sum + piece
    answer_sum = answer_sum.astype(bf16)

    def prefix_out(x):
        return x.transpose(1, 0, 2).reshape(prefix_keys.shape)

    def answer_out(x):
        return x.transpose(2, 1, 0, 3).reshape(answer_keys.shape)

    return (
        row_major(out_view),
        row_major(dq_view),
        answer_out(answer_sum[0]),
        answer_out(answer_sum[1]),
        prefix_out(prefix_sum[0]),
        prefix_out(prefix_sum[1]),
    )


def solution(mesh):
    wide = P("pair", "seq", None, "head")
    shared = P(("pair", "seq"), "head")
    small = P("pair", None)
    return jax.shard_map(
        on_device,
        mesh=mesh,
        in_specs=(wide, wide, wide, shared, shared, wide, small, small),
        out_specs=(wide, wide, wide, wide, shared, shared),
        check_vma=False,
    )
```

```python
import math

import jax
import jax.numpy as jnp
from jax import lax
from jax.experimental import pallas as pl
from jax.experimental.pallas import tpu as pltpu
from jax.sharding import PartitionSpec as P


HEAD_DIM = 128
NEGATIVE = -1e30
LOG2E = math.log2(math.e)

f32 = jnp.float32
bf16 = jnp.bfloat16
CHUNK = 32


def mm(a, b):
    return jnp.dot(a, b, preferred_element_type=f32)


def mm_nt(a, b):
    return lax.dot_general(a, b, (((1,), (1,)), ((), ())), preferred_element_type=f32)


def mm_tn(a, b):
    return lax.dot_general(a, b, (((0,), (0,)), ((), ())), preferred_element_type=f32)


def params(cells):
    limit = 24 if cells <= 2**20 else 60
    return pltpu.CompilerParams(
        dimension_semantics=("arbitrary",), vmem_limit_bytes=limit * 1024 * 1024
    )


def cost(flops, moved, exps):
    return pl.CostEstimate(flops=flops, bytes_accessed=moved, transcendentals=exps)


def place_prefix(refs, k_s, v_s):
    rows = refs[0].shape[-2]
    at = 0
    for ref in refs:
        for dz in range(ref.shape[0]):
            k_s[at : at + rows, :] = ref[dz, 0]
            if v_s is not None:
                v_s[at : at + rows, 0:HEAD_DIM] = ref[dz, 1]
            at += rows


def place_answer(refs, k_s, v_s):
    rows = refs[0].shape[-2]
    for t, ref in enumerate(refs):
        for b in range(ref.shape[1]):
            k_s[b, t * rows : (t + 1) * rows, :] = ref[0, b]
            v_s[b, t * rows : (t + 1) * rows, 0:HEAD_DIM] = ref[1, b]


def lanes(ref, here, update):
    for j in range(ref.shape[-1] // HEAD_DIM):
        columns = slice(j * HEAD_DIM, (j + 1) * HEAD_DIM)
        ref[0, here, columns] = update(columns)


def exponents(p_ref, s_s, m_s, first, rows):
    factor = HEAD_DIM ** (-0.5) * LOG2E

    def step(i, carry):
        here = pl.ds(pl.multiple_of(first + i * CHUNK, CHUNK), CHUNK)
        top = m_s(here)
        lanes(p_ref, here, lambda c: jnp.exp2(s_s[here, c] * factor - top).astype(bf16))
        return carry

    lax.fori_loop(0, rows // CHUNK, step, 0, unroll=7)


def blocks(total, rows, columns):
    size = total if total * columns <= 2**19 else rows
    return [slice(a, a + size) for a in range(0, total, size)]


def row_top(s):
    factor = HEAD_DIM ** (-0.5) * LOG2E
    top = jnp.max(s, axis=1, keepdims=True) * factor
    return jnp.broadcast_to(top, (s.shape[0], HEAD_DIM))


def score_grads(ds_s, p, dp, delta):
    for j in range(ds_s.shape[-1] // HEAD_DIM):
        columns = slice(j * HEAD_DIM, (j + 1) * HEAD_DIM)
        ds_s[:, columns] = (p[:, columns].astype(f32) * (dp[:, columns] - delta)).astype(bf16)


def prefix_forward_body(
    bias_ref, q_ref, pa_ref, pb_ref, pc_ref, pd_ref, p_ref, ol_ref, m_ref, k_s, v_s, s_s
):
    batch = bias_ref.shape[0]
    total = q_ref.shape[1]
    per = total // batch
    place_prefix((pa_ref, pb_ref, pc_ref, pd_ref), k_s, v_s)
    v_s[:, HEAD_DIM:] = jnp.ones((v_s.shape[0], HEAD_DIM), bf16)
    for b in range(batch):
        for part in blocks(per, 64, k_s.shape[0]):
            rows = slice(b * per + part.start, b * per + part.stop)
            s = mm_nt(q_ref[0, rows, :], k_s[...]) + bias_ref[b, 0:1, :]
            s_s[rows, :] = s
            m_ref[0, rows, :] = row_top(s)
    for b in range(batch):
        rows = slice(b * per, (b + 1) * per)
        exponents(p_ref, s_s, lambda here: m_ref[0, here, :], b * per, per)
        ol_ref[0, rows, :] = mm(p_ref[0, rows, :], v_s[...])


def middle_body(
    pieces,
    live_ref,
    bias_ref,
    q_ref,
    do_ref,
    p_ref,
    ol_ref,
    m_ref,
    *rest,
):
    prefix = rest[:4]
    answer = rest[4 : 4 + pieces]
    (
        out_ref,
        pb_ref,
        dob_ref,
        deltab_ref,
        ds_ref,
        own_ref,
        near_ref,
        far_ref,
        k_s,
        v_s,
        s_s,
        ka_s,
        va_s,
        olb_s,
        mb_s,
        doa_s,
        deltaa_s,
    ) = rest[4 + pieces :]
    scale = HEAD_DIM ** (-0.5)
    batch = ka_s.shape[0]
    keys = ka_s.shape[1]
    rows = bias_ref.shape[0]
    total = q_ref.shape[1]
    per = total // batch
    groups = per // rows
    place_answer(answer, ka_s, va_s)
    va_s[:, :, HEAD_DIM:] = jnp.ones((batch, keys, HEAD_DIM), bf16)
    place_prefix(prefix, k_s, v_s)
    for b in range(batch):
        for part in blocks(per, rows, keys):
            base = b * per + part.start
            size = part.stop - part.start
            scores = mm_nt(q_ref[0, base : base + size, :], ka_s[b])
            for g in range(size // rows):
                span = slice(base + g * rows, base + (g + 1) * rows)
                s = scores[g * rows : (g + 1) * rows, :] + bias_ref[...]
                s_s[span, :] = s
                mb_s[span, :] = row_top(s)
    for b in range(batch):
        exponents(pb_ref, s_s, lambda here: mb_s[here, :], b * per, per)
        olb_s[b * per : (b + 1) * per, :] = mm(pb_ref[0, b * per : (b + 1) * per, :], va_s[b])

    for b in range(batch):

        def combine(i, carry, b=b):
            here = pl.ds(pl.multiple_of(b * per + i * rows, rows), rows)
            live = live_ref[b]
            ma = m_ref[0, here, :]
            mb = mb_s[here, :]
            top = jnp.maximum(ma, mb)
            ea = jnp.exp2(ma - top)
            eb = jnp.exp2(mb - top)
            inverse = 1.0 / (
                ol_ref[0, here, HEAD_DIM:] * ea + olb_s[here, HEAD_DIM:] * eb
            )
            ea = ea * inverse
            eb = eb * inverse
            attended = (ol_ref[0, here, 0:HEAD_DIM] * ea + olb_s[here, 0:HEAD_DIM] * eb) * live
            out_ref[0, here, :] = attended.astype(bf16)
            douts = do_ref[0, here, :].astype(f32) * live
            da = (douts * ea).astype(bf16)
            db = (douts * eb).astype(bf16)
            doa_s[here, :] = da
            dob_ref[0, here, :] = db
            deltaa_s[here, :] = jnp.broadcast_to(
                jnp.sum(da.astype(f32) * attended, axis=1, keepdims=True), (rows, HEAD_DIM)
            )
            deltab_ref[0, here, :] = jnp.broadcast_to(
                jnp.sum(db.astype(f32) * attended, axis=1, keepdims=True), (rows, HEAD_DIM)
            )
            return carry

        lax.fori_loop(0, groups, combine, 0, unroll=groups)
    for span in blocks(total, per if per * k_s.shape[0] <= 2**19 else rows, k_s.shape[0]):
        dp = mm_nt(doa_s[span, :], v_s[...])
        score_grads(ds_ref.at[0, span], p_ref[0, span, :], dp, deltaa_s[span, :])
    half = own_ref.shape[1]
    quarter = half // 2
    value_term = jnp.transpose(mm_tn(doa_s[...], p_ref[0])).astype(bf16)
    key_term = (jnp.transpose(mm_tn(q_ref[0], ds_ref[0])) * scale).astype(bf16)
    for t, term in ((0, key_term), (1, value_term)):
        own_ref[t] = term[:half]
        near_ref[t] = term[half : half + quarter]
        far_ref[t] = term[half + quarter :]


def answer_backward_body(
    pieces, q_ref, ds_ref, pb_ref, dob_ref, deltab_ref, *rest
):
    prefix = rest[:4]
    rest = rest[4:]
    answer = rest[:pieces]
    dq_ref = rest[pieces]
    grads = rest[pieces + 1 : 2 * pieces + 1]
    k_s, ka_s, va_s, dsb_s = rest[2 * pieces + 1 :]
    scale = HEAD_DIM ** (-0.5)
    batch = ka_s.shape[0]
    total = q_ref.shape[1]
    per = total // batch
    piece_rows = answer[0].shape[-2]
    place_answer(answer, ka_s, va_s)
    place_prefix(prefix, k_s, None)
    for b in range(batch):
        for part in blocks(per, 64, ka_s.shape[1]):
            rows = slice(b * per + part.start, b * per + part.stop)
            dp = mm_nt(dob_ref[0, rows, :], va_s[b])
            score_grads(dsb_s.at[rows], pb_ref[0, rows, :], dp, deltab_ref[0, rows, :])
    for b in range(batch):
        rows = slice(b * per, (b + 1) * per)
        key_term = (jnp.transpose(mm_tn(q_ref[0, rows, :], dsb_s[rows, :])) * scale).astype(bf16)
        value_term = jnp.transpose(mm_tn(dob_ref[0, rows, :], pb_ref[0, rows, :])).astype(bf16)
        for t, ref in enumerate(grads):
            span = slice(t * piece_rows, (t + 1) * piece_rows)
            ref[0, b] = key_term[span]
            ref[1, b] = value_term[span]
    for b in range(batch):
        rows = slice(b * per, (b + 1) * per)
        dq = mm(ds_ref[0, rows, :], k_s[...]) + mm(dsb_s[rows, :], ka_s[b])
        dq_ref[0, rows, :] = (dq * scale).astype(bf16)


def on_device(
    queries,
    answer_keys,
    answer_values,
    prefix_keys,
    prefix_values,
    grad_out,
    answer_length,
    prefix_limit,
):
    size = lax.axis_size("seq")
    sides = lax.axis_size("pair")
    assert sides == 2 and size % 2 == 0
    outer = size // 2
    rows = queries.shape[1]
    batch = queries.shape[2]
    kv = answer_keys.shape[3] // HEAD_DIM
    group = queries.shape[3] // HEAD_DIM // kv
    per = group * rows
    total = batch * per
    prefix_rows = prefix_keys.shape[0]
    prefix_total = prefix_rows * size * sides
    answer_total = rows * size
    place = lax.axis_index("seq")
    side = lax.axis_index("pair")
    z, y = place // 2, place % 2

    def shift_z(x, k):
        return lax.ppermute(x, "seq", [(i, (i + 2 * k) % size) for i in range(size)])

    def swap_y(x):
        return lax.ppermute(x, "seq", [(i, i ^ 1) for i in range(size)])

    def swap_x(x):
        return lax.ppermute(x, "pair", [(0, 1), (1, 0)])

    prefix_own = jnp.stack([prefix_keys, prefix_values])
    answer_own = jnp.stack([a[0].transpose(1, 0, 2) for a in (answer_keys, answer_values)])
    prefix_z = jnp.stack([prefix_own] + [shift_z(prefix_own, k) for k in range(1, outer)])
    prefix_y = swap_y(prefix_z)
    prefix = [prefix_z, prefix_y, swap_x(prefix_z), swap_x(prefix_y)]
    near = [answer_own] + [shift_z(answer_own, k) for k in range(1, outer)]
    far = [swap_y(piece) for piece in near]
    answer = near + far
    pieces = len(answer)

    dz = jnp.arange(outer, dtype=jnp.int32)
    z_from = (z - dz) % outer
    pair_from = (side + jnp.arange(2, dtype=jnp.int32)) % 2
    y_from = (y + jnp.arange(2, dtype=jnp.int32)) % 2
    seq_from = z_from[None, :] * 2 + y_from[:, None]
    shard = pair_from[:, None, None] * size + seq_from[None]
    spots = (
        shard[..., None] * prefix_rows + jnp.arange(prefix_rows, dtype=jnp.int32)
    ).reshape(prefix_total)
    prefix_bias = jnp.where(spots[None, None, :] < prefix_limit[0][:, None, None], 0.0, NEGATIVE)
    prefix_bias = jnp.broadcast_to(prefix_bias, (batch, 8, prefix_total)).astype(f32)
    row_places = place * rows + jnp.arange(rows, dtype=jnp.int32)
    key_places = (
        seq_from[..., None] * rows + jnp.arange(rows, dtype=jnp.int32)
    ).reshape(answer_total)
    answer_bias = jnp.where(key_places[None, :] <= row_places[:, None], 0.0, NEGATIVE).astype(f32)
    live = jnp.where(row_places[None, :] < answer_length[0][:, None], 1.0, 0.0).astype(f32)
    live = jnp.broadcast_to(live[:, :, None], (batch, rows, HEAD_DIM))

    def head_major(x):
        x = x[0].reshape(rows, batch, kv, group, HEAD_DIM)
        return x.transpose(2, 1, 3, 0, 4).reshape(kv, total, HEAD_DIM)

    def row_major(x):
        x = x.reshape(kv, batch, group, rows, HEAD_DIM)
        return x.transpose(3, 1, 0, 2, 4).reshape(queries.shape)

    query_view = head_major(queries)
    grad_view = head_major(grad_out)

    def whole(shape):
        return pl.BlockSpec(shape, lambda c: (0,) * len(shape))

    def by_head(shape, axis=0):
        block = tuple(1 if a == axis else n for a, n in enumerate(shape))
        return pl.BlockSpec(block, lambda c: tuple(c if a == axis else 0 for a in range(len(shape))))

    def lane_block(shape):
        last = len(shape) - 1
        return pl.BlockSpec(shape[:-1] + (HEAD_DIM,), lambda c: (0,) * last + (c,))

    q_shape = (kv, total, HEAD_DIM)
    q_spec = by_head(q_shape)
    prefix_specs = [lane_block(prefix_z.shape)] * 4
    answer_spec = lane_block(answer_own.shape)
    pa_shape = (kv, total, prefix_total)
    pb_shape = (kv, total, answer_total)
    ol_shape = (kv, total, 2 * HEAD_DIM)
    own_shape = (2, prefix_total // 2, kv * HEAD_DIM)
    sent_shape = (2, prefix_total // 4, kv * HEAD_DIM)
    unit_a = 2 * kv * total * prefix_total * HEAD_DIM
    unit_b = 2 * kv * total * answer_total * HEAD_DIM

    probs_a, ol_a, top_a = pl.pallas_call(
        prefix_forward_body,
        grid=(kv,),
        in_specs=[whole(prefix_bias.shape), q_spec] + prefix_specs,
        out_specs=[by_head(pa_shape), by_head(ol_shape), q_spec],
        out_shape=[
            jax.ShapeDtypeStruct(pa_shape, bf16),
            jax.ShapeDtypeStruct(ol_shape, f32),
            jax.ShapeDtypeStruct(q_shape, f32),
        ],
        scratch_shapes=[
            pltpu.VMEM((prefix_total, HEAD_DIM), bf16),
            pltpu.VMEM((prefix_total, 2 * HEAD_DIM), bf16),
            pltpu.VMEM((total, prefix_total), f32),
        ],
        compiler_params=params(total * prefix_total),
        cost_estimate=cost(2 * unit_a, 8 << 20, kv * total * prefix_total),
        name="prefix_forward",
    )(prefix_bias, query_view, *prefix)

    (out_view, probs_b, grad_b, delta_b, ds_a, prefix_own_sum, prefix_near, prefix_far) = (
        pl.pallas_call(
            lambda *refs: middle_body(pieces, *refs),
            grid=(kv,),
            in_specs=[
                whole(live.shape),
                whole(answer_bias.shape),
                q_spec,
                q_spec,
                by_head(pa_shape),
                by_head(ol_shape),
                q_spec,
            ]
            + prefix_specs
            + [answer_spec] * pieces,
            out_specs=[
                q_spec,
                by_head(pb_shape),
                q_spec,
                q_spec,
                by_head(pa_shape),
                lane_block(own_shape),
                lane_block(sent_shape),
                lane_block(sent_shape),
            ],
            out_shape=[
                jax.ShapeDtypeStruct(q_shape, bf16),
                jax.ShapeDtypeStruct(pb_shape, bf16),
                jax.ShapeDtypeStruct(q_shape, bf16),
                jax.ShapeDtypeStruct(q_shape, f32),
                jax.ShapeDtypeStruct(pa_shape, bf16),
                jax.ShapeDtypeStruct(own_shape, bf16),
                jax.ShapeDtypeStruct(sent_shape, bf16),
                jax.ShapeDtypeStruct(sent_shape, bf16),
            ],
            scratch_shapes=[
                pltpu.VMEM((prefix_total, HEAD_DIM), bf16),
                pltpu.VMEM((prefix_total, HEAD_DIM), bf16),
                pltpu.VMEM((total, answer_total), f32),
                pltpu.VMEM((batch, answer_total, HEAD_DIM), bf16),
                pltpu.VMEM((batch, answer_total, 2 * HEAD_DIM), bf16),
                pltpu.VMEM((total, 2 * HEAD_DIM), f32),
                pltpu.VMEM((total, HEAD_DIM), f32),
                pltpu.VMEM((total, HEAD_DIM), bf16),
                pltpu.VMEM((total, HEAD_DIM), f32),
            ],
            compiler_params=params(total * prefix_total),
            cost_estimate=cost(2 * unit_b + 3 * unit_a, 12 << 20, kv * total * answer_total),
            name="middle",
        )(
            live,
            answer_bias,
            query_view,
            grad_view,
            probs_a,
            ol_a,
            top_a,
            *prefix,
            *answer,
        )
    )

    dq_view, *answer_grads = pl.pallas_call(
        lambda *refs: answer_backward_body(pieces, *refs),
        grid=(kv,),
        in_specs=[q_spec, by_head(pa_shape), by_head(pb_shape), q_spec, q_spec]
        + prefix_specs
        + [answer_spec] * pieces,
        out_specs=[q_spec] + [answer_spec] * pieces,
        out_shape=[jax.ShapeDtypeStruct(q_shape, bf16)]
        + [jax.ShapeDtypeStruct(answer_own.shape, bf16)] * pieces,
        scratch_shapes=[
            pltpu.VMEM((prefix_total, HEAD_DIM), bf16),
            pltpu.VMEM((batch, answer_total, HEAD_DIM), bf16),
            pltpu.VMEM((batch, answer_total, HEAD_DIM), bf16),
            pltpu.VMEM((total, answer_total), bf16),
        ],
        compiler_params=params(total * prefix_total),
        cost_estimate=cost(4 * unit_b + unit_a, 8 << 20, 0),
        name="answer_backward",
    )(query_view, ds_a, probs_b, grad_b, delta_b, *prefix, *answer)

    split = (2, outer, prefix_rows, kv * HEAD_DIM)
    half = prefix_total // 4
    far_got = swap_x(prefix_far).astype(f32) + prefix_own_sum[:, half:].astype(f32)
    y_got = swap_y(far_got.astype(bf16)).astype(f32)
    near_got = swap_x(prefix_near).astype(f32) + prefix_own_sum[:, :half].astype(f32)
    z_sum = (near_got + y_got).reshape(split)
    prefix_sum = z_sum[:, 0]
    for k in range(1, outer):
        prefix_sum = prefix_sum + shift_z(z_sum[:, k].astype(bf16), -k).astype(f32)
    answer_sum = None
    for k in reversed(range(outer)):
        got = swap_y(answer_grads[outer + k]).astype(f32)
        piece = answer_grads[k].astype(f32) + got
        if k:
            piece = shift_z(piece.astype(bf16), -k).astype(f32)
        answer_sum = piece if answer_sum is None else answer_sum + piece
    answer_sum = answer_sum.astype(bf16)

    def answer_out(x):
        return x.transpose(1, 0, 2).reshape(answer_keys.shape)

    attention_out = row_major(out_view)
    grad_queries = row_major(dq_view)
    return (
        attention_out,
        grad_queries,
        answer_out(answer_sum[0]),
        answer_out(answer_sum[1]),
        prefix_sum[0],
        prefix_sum[1],
    )


def solution(mesh):
    wide = P("pair", "seq", None, "head")
    shared = P(("pair", "seq"), "head")
    small = P("pair", None)

    return jax.shard_map(
        on_device,
        mesh=mesh,
        in_specs=(wide, wide, wide, shared, shared, wide, small, small),
        out_specs=(wide, wide, wide, wide, shared, shared),
        check_vma=False,
    )
```

```python
import math

import jax
import jax.numpy as jnp
from jax import lax
from jax.experimental import pallas as pl
from jax.experimental.layout import Layout, with_layout_constraint
from jax.experimental.pallas import tpu as pltpu
from jax.sharding import PartitionSpec as P


HEAD_DIM = 128
NEGATIVE = -1e30
LOG2E = math.log2(math.e)

f32 = jnp.float32
bf16 = jnp.bfloat16
CHUNK = 32


def mm(a, b):
    return jnp.dot(a, b, preferred_element_type=f32)


def mm_nt(a, b):
    return lax.dot_general(a, b, (((1,), (1,)), ((), ())), preferred_element_type=f32)


def mm_tn(a, b):
    return lax.dot_general(a, b, (((0,), (0,)), ((), ())), preferred_element_type=f32)


def params(cells):
    limit = 18 if cells <= 2**20 else 60
    return pltpu.CompilerParams(
        dimension_semantics=("arbitrary",), vmem_limit_bytes=limit * 1024 * 1024
    )


def cost(flops, moved, exps):
    return pl.CostEstimate(flops=flops, bytes_accessed=moved, transcendentals=exps)


def place_prefix(refs, k_s, v_s):
    rows = refs[0].shape[-2]
    at = 0
    for ref in refs:
        for dz in range(ref.shape[0]):
            k_s[at : at + rows, :] = ref[dz, 0]
            if v_s is not None:
                v_s[at : at + rows, 0:HEAD_DIM] = ref[dz, 1]
            at += rows


def place_answer(refs, k_s, v_s):
    rows = refs[0].shape[-2]
    for t, ref in enumerate(refs):
        for b in range(ref.shape[1]):
            k_s[b, t * rows : (t + 1) * rows, :] = ref[0, b]
            if v_s is not None:
                v_s[b, t * rows : (t + 1) * rows, 0:HEAD_DIM] = ref[1, b]


def lanes(ref, here, update):
    for j in range(ref.shape[-1] // HEAD_DIM):
        columns = slice(j * HEAD_DIM, (j + 1) * HEAD_DIM)
        ref[0, here, columns] = update(columns)


def exponents(p_ref, s_s, m_s, first, rows):
    factor = HEAD_DIM ** (-0.5) * LOG2E

    def step(i, carry):
        here = pl.ds(pl.multiple_of(first + i * CHUNK, CHUNK), CHUNK)
        top = m_s(here)
        lanes(p_ref, here, lambda c: jnp.exp2(s_s[here, c] * factor - top).astype(bf16))
        return carry

    lax.fori_loop(0, rows // CHUNK, step, 0, unroll=7)


def blocks(total, rows, columns):
    size = total if total * columns <= 2**19 else rows
    return [slice(a, a + size) for a in range(0, total, size)]


def row_top(s):
    factor = HEAD_DIM ** (-0.5) * LOG2E
    top = jnp.max(s, axis=1, keepdims=True) * factor
    return jnp.broadcast_to(top, (s.shape[0], HEAD_DIM))


def score_grads(ds_s, p, dp, delta):
    for j in range(ds_s.shape[-1] // HEAD_DIM):
        columns = slice(j * HEAD_DIM, (j + 1) * HEAD_DIM)
        ds_s[:, columns] = (p[:, columns].astype(f32) * (dp[:, columns] - delta)).astype(bf16)


def prefix_forward_body(
    bias_ref, q_ref, pa_ref, pb_ref, pc_ref, pd_ref, p_ref, ol_ref, m_ref, k_s, v_s, s_s
):
    batch = bias_ref.shape[0]
    total = q_ref.shape[1]
    per = total // batch
    place_prefix((pa_ref, pb_ref, pc_ref, pd_ref), k_s, v_s)
    v_s[:, HEAD_DIM:] = jnp.ones((v_s.shape[0], HEAD_DIM), bf16)
    for b in range(batch):
        for part in blocks(per, 64, k_s.shape[0]):
            rows = slice(b * per + part.start, b * per + part.stop)
            s = mm_nt(q_ref[0, rows, :], k_s[...]) + bias_ref[b, 0:1, :]
            s_s[rows, :] = s
            m_ref[0, rows, :] = row_top(s)
    for b in range(batch):
        rows = slice(b * per, (b + 1) * per)
        exponents(p_ref, s_s, lambda here: m_ref[0, here, :], b * per, per)
        ol_ref[0, rows, :] = mm(p_ref[0, rows, :], v_s[...])


def middle_body(
    pieces,
    live_ref,
    bias_ref,
    q_ref,
    do_ref,
    ol_ref,
    m_ref,
    *rest,
):
    answer = rest[:pieces]
    (
        out_ref,
        doa_ref,
        deltaa_ref,
        ds_ref,
        *grads,
        s_s,
        ka_s,
        va_s,
        olb_s,
        mb_s,
        p_s,
        dob_s,
        deltab_s,
    ) = rest[pieces:]
    scale = HEAD_DIM ** (-0.5)
    batch = ka_s.shape[0]
    keys = ka_s.shape[1]
    rows = bias_ref.shape[0]
    total = q_ref.shape[1]
    per = total // batch
    groups = per // rows
    piece_rows = answer[0].shape[-2]
    place_answer(answer, ka_s, va_s)
    va_s[:, :, HEAD_DIM:] = jnp.ones((batch, keys, HEAD_DIM), bf16)
    for b in range(batch):
        for part in blocks(per, rows, keys):
            base = b * per + part.start
            size = part.stop - part.start
            scores = mm_nt(q_ref[0, base : base + size, :], ka_s[b])
            for g in range(size // rows):
                span = slice(base + g * rows, base + (g + 1) * rows)
                s = scores[g * rows : (g + 1) * rows, :] + bias_ref[...]
                s_s[span, :] = s
                mb_s[span, :] = row_top(s)
    for b in range(batch):
        exponents(p_s, s_s, lambda here: mb_s[here, :], b * per, per)
        olb_s[b * per : (b + 1) * per, :] = mm(p_s[0, b * per : (b + 1) * per, :], va_s[b])

    for b in range(batch):

        def combine(i, carry, b=b):
            here = pl.ds(pl.multiple_of(b * per + i * rows, rows), rows)
            live = live_ref[b]
            ma = m_ref[0, here, :]
            mb = mb_s[here, :]
            top = jnp.maximum(ma, mb)
            ea = jnp.exp2(ma - top)
            eb = jnp.exp2(mb - top)
            inverse = 1.0 / (
                ol_ref[0, here, HEAD_DIM:] * ea + olb_s[here, HEAD_DIM:] * eb
            )
            ea = ea * inverse
            eb = eb * inverse
            attended = (ol_ref[0, here, 0:HEAD_DIM] * ea + olb_s[here, 0:HEAD_DIM] * eb) * live
            out_ref[0, here, :] = attended.astype(bf16)
            douts = do_ref[0, here, :].astype(f32) * live
            da = (douts * ea).astype(bf16)
            db = (douts * eb).astype(bf16)
            doa_ref[0, here, :] = da
            dob_s[here, :] = db
            deltaa_ref[0, here, :] = jnp.broadcast_to(
                jnp.sum(da.astype(f32) * attended, axis=1, keepdims=True), (rows, HEAD_DIM)
            )
            deltab_s[here, :] = jnp.broadcast_to(
                jnp.sum(db.astype(f32) * attended, axis=1, keepdims=True), (rows, HEAD_DIM)
            )
            return carry

        lax.fori_loop(0, groups, combine, 0, unroll=groups)
    for b in range(batch):
        for part in blocks(per, rows, keys):
            span = slice(b * per + part.start, b * per + part.stop)
            dp = mm_nt(dob_s[span, :], va_s[b, :, 0:HEAD_DIM])
            score_grads(ds_ref.at[0, span], p_s[0, span, :], dp, deltab_s[span, :])
    for b in range(batch):
        span = slice(b * per, (b + 1) * per)
        value_term = jnp.transpose(mm_tn(dob_s[span, :], p_s[0, span, :])).astype(bf16)
        key_term = (jnp.transpose(mm_tn(q_ref[0, span, :], ds_ref[0, span, :])) * scale).astype(bf16)
        for t in range(pieces):
            part = slice(t * piece_rows, (t + 1) * piece_rows)
            ref = grads[4 * t // pieces]
            ref[t % (pieces // 4), 0, b] = key_term[part]
            ref[t % (pieces // 4), 1, b] = value_term[part]


def prefix_backward_body(q_ref, p_ref, doa_ref, deltaa_ref, *rest):
    prefix = rest[:4]
    ds_ref, own_ref, near_ref, far_ref, k_s, v_s = rest[4:]
    scale = HEAD_DIM ** (-0.5)
    total = q_ref.shape[1]
    place_prefix(prefix, k_s, v_s)
    size = total // 2 if total // 2 * k_s.shape[0] <= 2**19 else 64
    for span in blocks(total, size, k_s.shape[0]):
        dp = mm_nt(doa_ref[0, span, :], v_s[...])
        score_grads(ds_ref.at[0, span], p_ref[0, span, :], dp, deltaa_ref[0, span, :])
    half = own_ref.shape[1]
    quarter = half // 2
    value_term = jnp.transpose(mm_tn(doa_ref[0], p_ref[0])).astype(bf16)
    key_term = (jnp.transpose(mm_tn(q_ref[0], ds_ref[0])) * scale).astype(bf16)
    for t, term in ((0, key_term), (1, value_term)):
        own_ref[t] = term[:half]
        near_ref[t] = term[half : half + quarter]
        far_ref[t] = term[half + quarter :]


def query_backward_body(pieces, dsa_ref, dsb_ref, *rest):
    prefix = rest[:4]
    answer = rest[4 : 4 + pieces]
    dq_ref, k_s, ka_s = rest[4 + pieces :]
    scale = HEAD_DIM ** (-0.5)
    batch = ka_s.shape[0]
    per = dq_ref.shape[1] // batch
    place_prefix(prefix, k_s, None)
    place_answer(answer, ka_s, None)
    for b in range(batch):
        rows = slice(b * per, (b + 1) * per)
        dq = mm(dsa_ref[0, rows, :], k_s[...]) + mm(dsb_ref[0, rows, :], ka_s[b])
        dq_ref[0, rows, :] = (dq * scale).astype(bf16)


def on_device(
    queries,
    answer_keys,
    answer_values,
    prefix_keys,
    prefix_values,
    grad_out,
    answer_length,
    prefix_limit,
):
    size = lax.axis_size("seq")
    sides = lax.axis_size("pair")
    assert sides == 2 and size >= 4 and size & (size - 1) == 0
    outer = size // 2
    rows = queries.shape[1]
    batch = queries.shape[2]
    kv = answer_keys.shape[3] // HEAD_DIM
    group = queries.shape[3] // HEAD_DIM // kv
    per = group * rows
    total = batch * per
    prefix_rows = prefix_keys.shape[0]
    prefix_total = prefix_rows * size * sides
    answer_total = rows * size
    place = lax.axis_index("seq")
    side = lax.axis_index("pair")
    z, y = place // 2, place % 2

    def swap_z(x, k):
        return lax.ppermute(x, "seq", [(i, i ^ (2 * k)) for i in range(size)])

    def swap_y(x):
        return lax.ppermute(x, "seq", [(i, i ^ 1) for i in range(size)])

    def swap_x(x):
        return lax.ppermute(x, "pair", [(0, 1), (1, 0)])

    prefix_own = jnp.stack([prefix_keys, prefix_values])
    answer_own = jnp.stack([a[0].transpose(1, 0, 2) for a in (answer_keys, answer_values)])
    prefix_z = jnp.stack([prefix_own] + [swap_z(prefix_own, k) for k in range(1, outer)])
    prefix_y = swap_y(prefix_z)
    prefix = [prefix_z, prefix_y, swap_x(prefix_z), swap_x(prefix_y)]
    near = [answer_own] + [swap_z(answer_own, k) for k in range(1, outer)]
    far = [swap_y(piece) for piece in near]
    answer = near + far
    pieces = len(answer)

    dz = jnp.arange(outer, dtype=jnp.int32)
    z_from = z ^ dz
    pair_from = (side + jnp.arange(2, dtype=jnp.int32)) % 2
    y_from = (y + jnp.arange(2, dtype=jnp.int32)) % 2
    seq_from = z_from[None, :] * 2 + y_from[:, None]
    shard = pair_from[:, None, None] * size + seq_from[None]
    spots = (
        shard[..., None] * prefix_rows + jnp.arange(prefix_rows, dtype=jnp.int32)
    ).reshape(prefix_total)
    prefix_bias = jnp.where(spots[None, None, :] < prefix_limit[0][:, None, None], 0.0, NEGATIVE)
    prefix_bias = jnp.broadcast_to(prefix_bias, (batch, 8, prefix_total)).astype(f32)
    row_places = place * rows + jnp.arange(rows, dtype=jnp.int32)
    key_places = (
        seq_from[..., None] * rows + jnp.arange(rows, dtype=jnp.int32)
    ).reshape(answer_total)
    answer_bias = jnp.where(key_places[None, :] <= row_places[:, None], 0.0, NEGATIVE).astype(f32)
    live = jnp.where(row_places[None, :] < answer_length[0][:, None], 1.0, 0.0).astype(f32)
    live = jnp.broadcast_to(live[:, :, None], (batch, rows, HEAD_DIM))

    def head_major(x):
        x = x[0].reshape(rows, batch, kv, group, HEAD_DIM)
        return x.transpose(2, 1, 3, 0, 4).reshape(kv, total, HEAD_DIM)

    def row_major(x):
        x = x.reshape(kv, batch, group, rows, HEAD_DIM)
        x = x.transpose(3, 1, 0, 2, 4).reshape(queries.shape)
        return with_layout_constraint(x, Layout((0, 1, 2, 3)))

    query_view = head_major(queries)
    grad_view = head_major(grad_out)

    def whole(shape):
        return pl.BlockSpec(shape, lambda c: (0,) * len(shape))

    def by_head(shape, axis=0):
        block = tuple(1 if a == axis else n for a, n in enumerate(shape))
        return pl.BlockSpec(block, lambda c: tuple(c if a == axis else 0 for a in range(len(shape))))

    def lane_block(shape):
        last = len(shape) - 1
        return pl.BlockSpec(shape[:-1] + (HEAD_DIM,), lambda c: (0,) * last + (c,))

    q_shape = (kv, total, HEAD_DIM)
    q_spec = by_head(q_shape)
    prefix_specs = [lane_block(prefix_z.shape)] * 4
    answer_spec = lane_block(answer_own.shape)
    pa_shape = (kv, total, prefix_total)
    pb_shape = (kv, total, answer_total)
    ol_shape = (kv, total, 2 * HEAD_DIM)
    own_shape = (2, prefix_total // 2, kv * HEAD_DIM)
    sent_shape = (2, prefix_total // 4, kv * HEAD_DIM)
    stack_shape = (outer // 2,) + answer_own.shape
    unit_a = 2 * kv * total * prefix_total * HEAD_DIM
    unit_b = 2 * kv * total * answer_total * HEAD_DIM

    probs_a, ol_a, top_a = pl.pallas_call(
        prefix_forward_body,
        grid=(kv,),
        in_specs=[whole(prefix_bias.shape), q_spec] + prefix_specs,
        out_specs=[by_head(pa_shape), by_head(ol_shape), q_spec],
        out_shape=[
            jax.ShapeDtypeStruct(pa_shape, bf16),
            jax.ShapeDtypeStruct(ol_shape, f32),
            jax.ShapeDtypeStruct(q_shape, f32),
        ],
        scratch_shapes=[
            pltpu.VMEM((prefix_total, HEAD_DIM), bf16),
            pltpu.VMEM((prefix_total, 2 * HEAD_DIM), bf16),
            pltpu.VMEM((total, prefix_total), f32),
        ],
        compiler_params=params(total * prefix_total),
        cost_estimate=cost(2 * unit_a, 8 << 20, kv * total * prefix_total),
        name="prefix_forward",
    )(prefix_bias, query_view, *prefix)

    (out_view, grad_a, delta_a, ds_b, near_low, near_high, far_low, far_high) = pl.pallas_call(
        lambda *refs: middle_body(pieces, *refs),
        grid=(kv,),
        in_specs=[
            whole(live.shape),
            whole(answer_bias.shape),
            q_spec,
            q_spec,
            by_head(ol_shape),
            q_spec,
        ]
        + [answer_spec] * pieces,
        out_specs=[q_spec, q_spec, q_spec, by_head(pb_shape)] + [lane_block(stack_shape)] * 4,
        out_shape=[
            jax.ShapeDtypeStruct(q_shape, bf16),
            jax.ShapeDtypeStruct(q_shape, bf16),
            jax.ShapeDtypeStruct(q_shape, f32),
            jax.ShapeDtypeStruct(pb_shape, bf16),
        ]
        + [jax.ShapeDtypeStruct(stack_shape, bf16)] * 4,
        scratch_shapes=[
            pltpu.VMEM((total, answer_total), f32),
            pltpu.VMEM((batch, answer_total, HEAD_DIM), bf16),
            pltpu.VMEM((batch, answer_total, 2 * HEAD_DIM), bf16),
            pltpu.VMEM((total, 2 * HEAD_DIM), f32),
            pltpu.VMEM((total, HEAD_DIM), f32),
            pltpu.VMEM((1, total, answer_total), bf16),
            pltpu.VMEM((total, HEAD_DIM), bf16),
            pltpu.VMEM((total, HEAD_DIM), f32),
        ],
        compiler_params=params(total * prefix_total),
        cost_estimate=cost(5 * unit_b, 12 << 20, kv * total * answer_total),
        name="middle",
    )(live, answer_bias, query_view, grad_view, ol_a, top_a, *answer)

    ds_a, prefix_own_sum, prefix_near, prefix_far = pl.pallas_call(
        prefix_backward_body,
        grid=(kv,),
        in_specs=[q_spec, by_head(pa_shape), q_spec, q_spec] + prefix_specs,
        out_specs=[
            by_head(pa_shape),
            lane_block(own_shape),
            lane_block(sent_shape),
            lane_block(sent_shape),
        ],
        out_shape=[
            jax.ShapeDtypeStruct(pa_shape, bf16),
            jax.ShapeDtypeStruct(own_shape, bf16),
            jax.ShapeDtypeStruct(sent_shape, bf16),
            jax.ShapeDtypeStruct(sent_shape, bf16),
        ],
        scratch_shapes=[
            pltpu.VMEM((prefix_total, HEAD_DIM), bf16),
            pltpu.VMEM((prefix_total, HEAD_DIM), bf16),
        ],
        compiler_params=params(total * prefix_total),
        cost_estimate=cost(3 * unit_a, 12 << 20, 0),
        name="prefix_backward",
    )(query_view, probs_a, grad_a, delta_a, *prefix)

    dq_view = pl.pallas_call(
        lambda *refs: query_backward_body(pieces, *refs),
        grid=(kv,),
        in_specs=[by_head(pa_shape), by_head(pb_shape)] + prefix_specs + [answer_spec] * pieces,
        out_specs=q_spec,
        out_shape=jax.ShapeDtypeStruct(q_shape, bf16),
        scratch_shapes=[
            pltpu.VMEM((prefix_total, HEAD_DIM), bf16),
            pltpu.VMEM((batch, answer_total, HEAD_DIM), bf16),
        ],
        compiler_params=params(total * prefix_total),
        cost_estimate=cost(unit_a + unit_b, 8 << 20, 0),
        name="query_backward",
    )(ds_a, ds_b, *prefix, *answer)

    split = (2, outer, prefix_rows, kv * HEAD_DIM)
    half = prefix_total // 4
    far_got = swap_x(prefix_far).astype(f32) + prefix_own_sum[:, half:].astype(f32)
    y_got = swap_y(far_got.astype(bf16)).astype(f32)
    near_got = swap_x(prefix_near).astype(f32) + prefix_own_sum[:, :half].astype(f32)
    z_sum = (near_got + y_got).reshape(split)
    prefix_sum = z_sum[:, 0]
    for k in range(1, outer):
        prefix_sum = prefix_sum + swap_z(z_sum[:, k].astype(bf16), k).astype(f32)
    high_got = swap_y(far_high)
    low_got = swap_y(far_low)
    high = (near_high.astype(f32) + high_got.astype(f32)).astype(bf16)
    low = near_low.astype(f32) + low_got.astype(f32)
    answer_sum = low[0]
    for k in range(1, outer):
        at = k % (outer // 2)
        piece = (high if k >= outer // 2 else low)[at]
        answer_sum = answer_sum + swap_z(piece.astype(bf16), k).astype(f32)
    answer_sum = answer_sum.astype(bf16)

    def answer_out(x):
        return x.transpose(1, 0, 2).reshape(answer_keys.shape)

    attention_out = row_major(out_view)
    grad_queries = row_major(dq_view)
    return (
        attention_out,
        grad_queries,
        answer_out(answer_sum[0]),
        answer_out(answer_sum[1]),
        prefix_sum[0],
        prefix_sum[1],
    )


def solution(mesh):
    wide = P("pair", "seq", None, "head")
    shared = P(("pair", "seq"), "head")
    small = P("pair", None)

    return jax.shard_map(
        on_device,
        mesh=mesh,
        in_specs=(wide, wide, wide, shared, shared, wide, small, small),
        out_specs=(wide, wide, wide, wide, shared, shared),
        check_vma=False,
    )
```

```python
import math

import jax
import jax.numpy as jnp
from jax import lax
from jax.experimental import pallas as pl
from jax.experimental.pallas import tpu as pltpu
from jax.sharding import PartitionSpec as P


HEAD_DIM = 128
NEGATIVE = -1e30
LOG2E = math.log2(math.e)

f32 = jnp.float32
bf16 = jnp.bfloat16
CHUNK = 32


def mm(a, b):
    return jnp.dot(a, b, preferred_element_type=f32)


def mm_nt(a, b):
    return lax.dot_general(a, b, (((1,), (1,)), ((), ())), preferred_element_type=f32)


def mm_tn(a, b):
    return lax.dot_general(a, b, (((0,), (0,)), ((), ())), preferred_element_type=f32)


def params(cells):
    limit = 18 if cells <= 2**20 else 60
    return pltpu.CompilerParams(
        dimension_semantics=("arbitrary",), vmem_limit_bytes=limit * 1024 * 1024
    )


def cost(flops, moved, exps):
    return pl.CostEstimate(flops=flops, bytes_accessed=moved, transcendentals=exps)


def place_prefix(refs, k_s, v_s):
    rows = refs[0].shape[-2]
    at = 0
    for ref in refs:
        for dz in range(ref.shape[0]):
            k_s[at : at + rows, :] = ref[dz, 0]
            if v_s is not None:
                v_s[at : at + rows, 0:HEAD_DIM] = ref[dz, 1]
            at += rows


def place_answer(refs, k_s, v_s):
    rows = refs[0].shape[-2]
    for t, ref in enumerate(refs):
        for b in range(ref.shape[1]):
            k_s[b, t * rows : (t + 1) * rows, :] = ref[0, b]
            if v_s is not None:
                v_s[b, t * rows : (t + 1) * rows, 0:HEAD_DIM] = ref[1, b]


def lanes(ref, here, update):
    for j in range(ref.shape[-1] // HEAD_DIM):
        columns = slice(j * HEAD_DIM, (j + 1) * HEAD_DIM)
        ref[0, here, columns] = update(columns)


def exponents(p_ref, s_s, m_s, first, rows):
    factor = HEAD_DIM ** (-0.5) * LOG2E

    def step(i, carry):
        here = pl.ds(pl.multiple_of(first + i * CHUNK, CHUNK), CHUNK)
        top = m_s(here)
        lanes(p_ref, here, lambda c: jnp.exp2(s_s[here, c] * factor - top).astype(bf16))
        return carry

    small = rows * s_s.shape[1] <= 2**19
    lax.fori_loop(0, rows // CHUNK, step, 0, unroll=rows // CHUNK if small else 7)


def blocks(total, rows, columns):
    size = total if total * columns <= 2**19 else rows
    return [slice(a, a + size) for a in range(0, total, size)]


def row_top(s):
    factor = HEAD_DIM ** (-0.5) * LOG2E
    top = jnp.max(s, axis=1, keepdims=True) * factor
    return jnp.broadcast_to(top, (s.shape[0], HEAD_DIM))


def score_grads(ds_s, p, dp, delta):
    for j in range(ds_s.shape[-1] // HEAD_DIM):
        columns = slice(j * HEAD_DIM, (j + 1) * HEAD_DIM)
        ds_s[:, columns] = (p[:, columns].astype(f32) * (dp[:, columns] - delta)).astype(bf16)


def interleave(rows, batch):
    size = rows * batch
    at = lax.broadcasted_iota(jnp.int32, (size, size), 0)
    source = lax.broadcasted_iota(jnp.int32, (size, size), 1)
    return jnp.where(source == (at % rows) * batch + at // rows, 1.0, 0.0).astype(bf16)


def gather_rows(raw_ref, out):
    _, rows, batch, width = raw_ref.shape
    select = interleave(rows, batch)
    group = width // HEAD_DIM
    for g in range(group):
        x = raw_ref[0, :, :, g * HEAD_DIM : (g + 1) * HEAD_DIM].reshape(rows * batch, HEAD_DIM)
        x = mm(select, x).astype(bf16)
        for b in range(batch):
            at = (b * group + g) * rows
            out[at : at + rows, :] = x[b * rows : (b + 1) * rows]


def scatter_rows(view, raw_ref):
    _, rows, batch, width = raw_ref.shape
    select = interleave(rows, batch)
    group = width // HEAD_DIM
    for g in range(group):
        spans = [(b * group + g) * rows for b in range(batch)]
        x = jnp.concatenate([view[at : at + rows, :] for at in spans], axis=0)
        x = mm_tn(select, x).astype(bf16)
        raw_ref[0, :, :, g * HEAD_DIM : (g + 1) * HEAD_DIM] = x.reshape(rows, batch, HEAD_DIM)


def arrange_body(raw_q_ref, raw_do_ref, q_ref, do_ref):
    gather_rows(raw_q_ref, q_ref.at[0])
    gather_rows(raw_do_ref, do_ref.at[0])


def prefix_forward_body(
    bias_ref, q_ref, pa_ref, pb_ref, pc_ref, pd_ref, p_ref, ol_ref, m_ref, k_s, v_s, s_s
):
    batch = bias_ref.shape[0]
    total = q_ref.shape[1]
    per = total // batch
    place_prefix((pa_ref, pb_ref, pc_ref, pd_ref), k_s, v_s)
    v_s[:, HEAD_DIM:] = jnp.ones((v_s.shape[0], HEAD_DIM), bf16)
    for b in range(batch):
        for part in blocks(per, 64, k_s.shape[0]):
            rows = slice(b * per + part.start, b * per + part.stop)
            s = mm_nt(q_ref[0, rows, :], k_s[...]) + bias_ref[b, 0:1, :]
            s_s[rows, :] = s
            m_ref[0, rows, :] = row_top(s)
    for b in range(batch):
        rows = slice(b * per, (b + 1) * per)
        exponents(p_ref, s_s, lambda here: m_ref[0, here, :], b * per, per)
        ol_ref[0, rows, :] = mm(p_ref[0, rows, :], v_s[...])


def middle_body(
    pieces,
    live_ref,
    bias_ref,
    q_ref,
    do_ref,
    ol_ref,
    m_ref,
    *rest,
):
    answer = rest[:pieces]
    (
        out_ref,
        doa_ref,
        deltaa_ref,
        ds_ref,
        *grads,
        s_s,
        ka_s,
        va_s,
        olb_s,
        mb_s,
        p_s,
        dob_s,
        deltab_s,
    ) = rest[pieces:]
    scale = HEAD_DIM ** (-0.5)
    batch = ka_s.shape[0]
    keys = ka_s.shape[1]
    rows = bias_ref.shape[0]
    total = q_ref.shape[1]
    per = total // batch
    groups = per // rows
    piece_rows = answer[0].shape[-2]
    place_answer(answer, ka_s, va_s)
    va_s[:, :, HEAD_DIM:] = jnp.ones((batch, keys, HEAD_DIM), bf16)
    for b in range(batch):
        for part in blocks(per, rows, keys):
            base = b * per + part.start
            size = part.stop - part.start
            scores = mm_nt(q_ref[0, base : base + size, :], ka_s[b])
            for g in range(size // rows):
                span = slice(base + g * rows, base + (g + 1) * rows)
                s = scores[g * rows : (g + 1) * rows, :] + bias_ref[...]
                s_s[span, :] = s
                mb_s[span, :] = row_top(s)
    for b in range(batch):
        exponents(p_s, s_s, lambda here: mb_s[here, :], b * per, per)
        olb_s[b * per : (b + 1) * per, :] = mm(p_s[0, b * per : (b + 1) * per, :], va_s[b])

    for b in range(batch):

        def combine(i, carry, b=b):
            here = pl.ds(pl.multiple_of(b * per + i * rows, rows), rows)
            live = live_ref[b]
            ma = m_ref[0, here, :]
            mb = mb_s[here, :]
            top = jnp.maximum(ma, mb)
            ea = jnp.exp2(ma - top)
            eb = jnp.exp2(mb - top)
            inverse = 1.0 / (
                ol_ref[0, here, HEAD_DIM:] * ea + olb_s[here, HEAD_DIM:] * eb
            )
            ea = ea * inverse
            eb = eb * inverse
            attended = (ol_ref[0, here, 0:HEAD_DIM] * ea + olb_s[here, 0:HEAD_DIM] * eb) * live
            out_ref[0, here, :] = attended.astype(bf16)
            douts = do_ref[0, here, :].astype(f32) * live
            da = (douts * ea).astype(bf16)
            db = (douts * eb).astype(bf16)
            doa_ref[0, here, :] = da
            dob_s[here, :] = db
            deltaa_ref[0, here, :] = jnp.broadcast_to(
                jnp.sum(da.astype(f32) * attended, axis=1, keepdims=True), (rows, HEAD_DIM)
            )
            deltab_s[here, :] = jnp.broadcast_to(
                jnp.sum(db.astype(f32) * attended, axis=1, keepdims=True), (rows, HEAD_DIM)
            )
            return carry

        lax.fori_loop(0, groups, combine, 0, unroll=groups)
    for b in range(batch):
        for part in blocks(per, rows, keys):
            span = slice(b * per + part.start, b * per + part.stop)
            dp = mm_nt(dob_s[span, :], va_s[b, :, 0:HEAD_DIM])
            score_grads(ds_ref.at[0, span], p_s[0, span, :], dp, deltab_s[span, :])
    for b in range(batch):
        span = slice(b * per, (b + 1) * per)
        value_term = jnp.transpose(mm_tn(dob_s[span, :], p_s[0, span, :])).astype(bf16)
        key_term = (jnp.transpose(mm_tn(q_ref[0, span, :], ds_ref[0, span, :])) * scale).astype(bf16)
        for t in range(pieces):
            part = slice(t * piece_rows, (t + 1) * piece_rows)
            ref = grads[4 * t // pieces]
            ref[t % (pieces // 4), 0, b] = key_term[part]
            ref[t % (pieces // 4), 1, b] = value_term[part]


def prefix_backward_body(q_ref, p_ref, doa_ref, deltaa_ref, *rest):
    prefix = rest[:4]
    ds_ref, own_ref, near_ref, far_ref, k_s, v_s = rest[4:]
    scale = HEAD_DIM ** (-0.5)
    total = q_ref.shape[1]
    place_prefix(prefix, k_s, v_s)
    size = total // 2 if total // 2 * k_s.shape[0] <= 2**19 else 64
    for span in blocks(total, size, k_s.shape[0]):
        dp = mm_nt(doa_ref[0, span, :], v_s[...])
        score_grads(ds_ref.at[0, span], p_ref[0, span, :], dp, deltaa_ref[0, span, :])
    half = own_ref.shape[1]
    quarter = half // 2
    value_term = jnp.transpose(mm_tn(doa_ref[0], p_ref[0])).astype(bf16)
    key_term = (jnp.transpose(mm_tn(q_ref[0], ds_ref[0])) * scale).astype(bf16)
    for t, term in ((0, key_term), (1, value_term)):
        own_ref[t] = term[:half]
        near_ref[t] = term[half : half + quarter]
        far_ref[t] = term[half + quarter :]


def query_backward_body(pieces, out_ref, dsa_ref, dsb_ref, *rest):
    prefix = rest[:4]
    answer = rest[4 : 4 + pieces]
    raw_out_ref, raw_dq_ref, k_s, ka_s, dq_s = rest[4 + pieces :]
    scale = HEAD_DIM ** (-0.5)
    batch = ka_s.shape[0]
    per = dq_s.shape[0] // batch
    place_prefix(prefix, k_s, None)
    place_answer(answer, ka_s, None)
    for b in range(batch):
        rows = slice(b * per, (b + 1) * per)
        dq = mm(dsa_ref[0, rows, :], k_s[...]) + mm(dsb_ref[0, rows, :], ka_s[b])
        dq_s[rows, :] = (dq * scale).astype(bf16)
    scatter_rows(out_ref.at[0], raw_out_ref)
    scatter_rows(dq_s, raw_dq_ref)


def on_device(
    queries,
    answer_keys,
    answer_values,
    prefix_keys,
    prefix_values,
    grad_out,
    answer_length,
    prefix_limit,
):
    size = lax.axis_size("seq")
    sides = lax.axis_size("pair")
    assert sides == 2 and size >= 4 and size & (size - 1) == 0
    outer = size // 2
    rows = queries.shape[1]
    batch = queries.shape[2]
    kv = answer_keys.shape[3] // HEAD_DIM
    group = queries.shape[3] // HEAD_DIM // kv
    per = group * rows
    total = batch * per
    prefix_rows = prefix_keys.shape[0]
    prefix_total = prefix_rows * size * sides
    answer_total = rows * size
    place = lax.axis_index("seq")
    side = lax.axis_index("pair")
    z, y = place // 2, place % 2

    def swap_z(x, k):
        return lax.ppermute(x, "seq", [(i, i ^ (2 * k)) for i in range(size)])

    def swap_y(x):
        return lax.ppermute(x, "seq", [(i, i ^ 1) for i in range(size)])

    def swap_x(x):
        return lax.ppermute(x, "pair", [(0, 1), (1, 0)])

    prefix_own = jnp.stack([prefix_keys, prefix_values])
    answer_own = jnp.stack([a[0].transpose(1, 0, 2) for a in (answer_keys, answer_values)])
    prefix_z = jnp.stack([prefix_own] + [swap_z(prefix_own, k) for k in range(1, outer)])
    prefix_y = swap_y(prefix_z)
    prefix = [prefix_z, prefix_y, swap_x(prefix_z), swap_x(prefix_y)]
    near = [answer_own] + [swap_z(answer_own, k) for k in range(1, outer)]
    far = [swap_y(piece) for piece in near]
    answer = near + far
    pieces = len(answer)

    dz = jnp.arange(outer, dtype=jnp.int32)
    z_from = z ^ dz
    pair_from = (side + jnp.arange(2, dtype=jnp.int32)) % 2
    y_from = (y + jnp.arange(2, dtype=jnp.int32)) % 2
    seq_from = z_from[None, :] * 2 + y_from[:, None]
    shard = pair_from[:, None, None] * size + seq_from[None]
    spots = (
        shard[..., None] * prefix_rows + jnp.arange(prefix_rows, dtype=jnp.int32)
    ).reshape(prefix_total)
    prefix_bias = jnp.where(spots[None, None, :] < prefix_limit[0][:, None, None], 0.0, NEGATIVE)
    prefix_bias = jnp.broadcast_to(prefix_bias, (batch, 8, prefix_total)).astype(f32)
    row_places = place * rows + jnp.arange(rows, dtype=jnp.int32)
    key_places = (
        seq_from[..., None] * rows + jnp.arange(rows, dtype=jnp.int32)
    ).reshape(answer_total)
    answer_bias = jnp.where(key_places[None, :] <= row_places[:, None], 0.0, NEGATIVE).astype(f32)
    live = jnp.where(row_places[None, :] < answer_length[0][:, None], 1.0, 0.0).astype(f32)
    live = jnp.broadcast_to(live[:, :, None], (batch, rows, HEAD_DIM))

    def whole(shape):
        return pl.BlockSpec(shape, lambda c: (0,) * len(shape))

    def by_head(shape, axis=0):
        block = tuple(1 if a == axis else n for a, n in enumerate(shape))
        return pl.BlockSpec(block, lambda c: tuple(c if a == axis else 0 for a in range(len(shape))))

    def lane_block(shape):
        last = len(shape) - 1
        return pl.BlockSpec(shape[:-1] + (HEAD_DIM,), lambda c: (0,) * last + (c,))

    raw_spec = pl.BlockSpec((1, rows, batch, group * HEAD_DIM), lambda c: (0, 0, 0, c))
    q_shape = (kv, total, HEAD_DIM)
    q_spec = by_head(q_shape)
    prefix_specs = [lane_block(prefix_z.shape)] * 4
    answer_spec = lane_block(answer_own.shape)
    pa_shape = (kv, total, prefix_total)
    pb_shape = (kv, total, answer_total)
    ol_shape = (kv, total, 2 * HEAD_DIM)
    own_shape = (2, prefix_total // 2, kv * HEAD_DIM)
    sent_shape = (2, prefix_total // 4, kv * HEAD_DIM)
    stack_shape = (outer // 2,) + answer_own.shape
    unit_a = 2 * kv * total * prefix_total * HEAD_DIM
    unit_b = 2 * kv * total * answer_total * HEAD_DIM

    query_view, grad_view = pl.pallas_call(
        arrange_body,
        grid=(kv,),
        in_specs=[raw_spec, raw_spec],
        out_specs=[q_spec, q_spec],
        out_shape=[jax.ShapeDtypeStruct(q_shape, bf16)] * 2,
        compiler_params=params(total * prefix_total),
        cost_estimate=cost(4 * kv * total * HEAD_DIM * HEAD_DIM, 4 << 20, 0),
        name="arrange",
    )(queries, grad_out)

    probs_a, ol_a, top_a = pl.pallas_call(
        prefix_forward_body,
        grid=(kv,),
        in_specs=[whole(prefix_bias.shape), q_spec] + prefix_specs,
        out_specs=[by_head(pa_shape), by_head(ol_shape), q_spec],
        out_shape=[
            jax.ShapeDtypeStruct(pa_shape, bf16),
            jax.ShapeDtypeStruct(ol_shape, f32),
            jax.ShapeDtypeStruct(q_shape, f32),
        ],
        scratch_shapes=[
            pltpu.VMEM((prefix_total, HEAD_DIM), bf16),
            pltpu.VMEM((prefix_total, 2 * HEAD_DIM), bf16),
            pltpu.VMEM((total, prefix_total), f32),
        ],
        compiler_params=params(total * prefix_total),
        cost_estimate=cost(2 * unit_a, 8 << 20, kv * total * prefix_total),
        name="prefix_forward",
    )(prefix_bias, query_view, *prefix)

    (out_view, grad_a, delta_a, ds_b, near_low, near_high, far_low, far_high) = pl.pallas_call(
        lambda *refs: middle_body(pieces, *refs),
        grid=(kv,),
        in_specs=[
            whole(live.shape),
            whole(answer_bias.shape),
            q_spec,
            q_spec,
            by_head(ol_shape),
            q_spec,
        ]
        + [answer_spec] * pieces,
        out_specs=[q_spec, q_spec, q_spec, by_head(pb_shape)] + [lane_block(stack_shape)] * 4,
        out_shape=[
            jax.ShapeDtypeStruct(q_shape, bf16),
            jax.ShapeDtypeStruct(q_shape, bf16),
            jax.ShapeDtypeStruct(q_shape, f32),
            jax.ShapeDtypeStruct(pb_shape, bf16),
        ]
        + [jax.ShapeDtypeStruct(stack_shape, bf16)] * 4,
        scratch_shapes=[
            pltpu.VMEM((total, answer_total), f32),
            pltpu.VMEM((batch, answer_total, HEAD_DIM), bf16),
            pltpu.VMEM((batch, answer_total, 2 * HEAD_DIM), bf16),
            pltpu.VMEM((total, 2 * HEAD_DIM), f32),
            pltpu.VMEM((total, HEAD_DIM), f32),
            pltpu.VMEM((1, total, answer_total), bf16),
            pltpu.VMEM((total, HEAD_DIM), bf16),
            pltpu.VMEM((total, HEAD_DIM), f32),
        ],
        compiler_params=params(total * prefix_total),
        cost_estimate=cost(5 * unit_b, 12 << 20, kv * total * answer_total),
        name="middle",
    )(live, answer_bias, query_view, grad_view, ol_a, top_a, *answer)

    ds_a, prefix_own_sum, prefix_near, prefix_far = pl.pallas_call(
        prefix_backward_body,
        grid=(kv,),
        in_specs=[q_spec, by_head(pa_shape), q_spec, q_spec] + prefix_specs,
        out_specs=[
            by_head(pa_shape),
            lane_block(own_shape),
            lane_block(sent_shape),
            lane_block(sent_shape),
        ],
        out_shape=[
            jax.ShapeDtypeStruct(pa_shape, bf16),
            jax.ShapeDtypeStruct(own_shape, bf16),
            jax.ShapeDtypeStruct(sent_shape, bf16),
            jax.ShapeDtypeStruct(sent_shape, bf16),
        ],
        scratch_shapes=[
            pltpu.VMEM((prefix_total, HEAD_DIM), bf16),
            pltpu.VMEM((prefix_total, HEAD_DIM), bf16),
        ],
        compiler_params=params(total * prefix_total),
        cost_estimate=cost(3 * unit_a, 12 << 20, 0),
        name="prefix_backward",
    )(query_view, probs_a, grad_a, delta_a, *prefix)

    attention_out, grad_queries = pl.pallas_call(
        lambda *refs: query_backward_body(pieces, *refs),
        grid=(kv,),
        in_specs=[q_spec, by_head(pa_shape), by_head(pb_shape)]
        + prefix_specs
        + [answer_spec] * pieces,
        out_specs=[raw_spec, raw_spec],
        out_shape=[jax.ShapeDtypeStruct(queries.shape, bf16)] * 2,
        scratch_shapes=[
            pltpu.VMEM((prefix_total, HEAD_DIM), bf16),
            pltpu.VMEM((batch, answer_total, HEAD_DIM), bf16),
            pltpu.VMEM((total, HEAD_DIM), bf16),
        ],
        compiler_params=params(total * prefix_total),
        cost_estimate=cost(unit_a + unit_b, 8 << 20, 0),
        name="query_backward",
    )(out_view, ds_a, ds_b, *prefix, *answer)

    split = (2, outer, prefix_rows, kv * HEAD_DIM)
    half = prefix_total // 4
    far_got = swap_x(prefix_far).astype(f32) + prefix_own_sum[:, half:].astype(f32)
    y_got = swap_y(far_got.astype(bf16)).astype(f32)
    near_got = swap_x(prefix_near).astype(f32)
    z_sum = (near_got + prefix_own_sum[:, :half].astype(f32) + y_got).reshape(split)
    prefix_sum = z_sum[:, 0]
    for k in range(1, outer):
        prefix_sum = prefix_sum + swap_z(z_sum[:, k].astype(bf16), k).astype(f32)
    high_got = swap_y(far_high)
    low_got = swap_y(far_low)
    high = (near_high.astype(f32) + high_got.astype(f32)).astype(bf16)
    low = near_low.astype(f32) + low_got.astype(f32)
    answer_sum = low[0]
    for k in range(1, outer):
        at = k % (outer // 2)
        piece = (high if k >= outer // 2 else low)[at]
        answer_sum = answer_sum + swap_z(piece.astype(bf16), k).astype(f32)
    answer_sum = answer_sum.astype(bf16)

    def answer_out(x):
        return x.transpose(1, 0, 2).reshape(answer_keys.shape)

    return (
        attention_out,
        grad_queries,
        answer_out(answer_sum[0]),
        answer_out(answer_sum[1]),
        prefix_sum[0],
        prefix_sum[1],
    )


def solution(mesh):
    wide = P("pair", "seq", None, "head")
    shared = P(("pair", "seq"), "head")
    small = P("pair", None)

    return jax.shard_map(
        on_device,
        mesh=mesh,
        in_specs=(wide, wide, wide, shared, shared, wide, small, small),
        out_specs=(wide, wide, wide, wide, shared, shared),
        check_vma=False,
    )
```

```python
import math

import jax
import jax.numpy as jnp
from jax import lax
from jax.experimental import pallas as pl
from jax.experimental.pallas import tpu as pltpu
from jax.sharding import PartitionSpec as P


HEAD_DIM = 128
NEGATIVE = -1e30
LOG2E = math.log2(math.e)

f32 = jnp.float32
bf16 = jnp.bfloat16
CHUNK = 32


def mm(a, b):
    return jnp.dot(a, b, preferred_element_type=f32)


def mm_nt(a, b):
    return lax.dot_general(a, b, (((1,), (1,)), ((), ())), preferred_element_type=f32)


def mm_tn(a, b):
    return lax.dot_general(a, b, (((0,), (0,)), ((), ())), preferred_element_type=f32)


def params(cells):
    limit = 18 if cells <= 2**20 else 60
    return pltpu.CompilerParams(
        dimension_semantics=("arbitrary",), vmem_limit_bytes=limit * 1024 * 1024
    )


def cost(flops, moved, exps):
    return pl.CostEstimate(flops=flops, bytes_accessed=moved, transcendentals=exps)


def head_columns():
    return pl.ds(pl.multiple_of(pl.program_id(0) * HEAD_DIM, HEAD_DIM), HEAD_DIM)


def place_prefix(refs, k_s, v_s):
    columns = head_columns()
    rows = refs[0].shape[-2]
    at = 0
    for ref in refs:
        for dz in range(ref.shape[0]):
            k_s[at : at + rows, :] = ref[dz, 0, :, columns]
            if v_s is not None:
                v_s[at : at + rows, 0:HEAD_DIM] = ref[dz, 1, :, columns]
            at += rows


def place_answer(refs, k_s, v_s):
    columns = head_columns()
    rows = refs[0].shape[-2]
    for t, ref in enumerate(refs):
        for b in range(ref.shape[1]):
            k_s[b, t * rows : (t + 1) * rows, :] = ref[0, b, :, columns]
            if v_s is not None:
                v_s[b, t * rows : (t + 1) * rows, 0:HEAD_DIM] = ref[1, b, :, columns]


def lanes(ref, here, update):
    for j in range(ref.shape[-1] // HEAD_DIM):
        columns = slice(j * HEAD_DIM, (j + 1) * HEAD_DIM)
        ref[0, here, columns] = update(columns)


def exponents(p_ref, s_s, m_s, first, rows):
    factor = HEAD_DIM ** (-0.5) * LOG2E

    def step(i, carry):
        here = pl.ds(pl.multiple_of(first + i * CHUNK, CHUNK), CHUNK)
        top = m_s(here)
        lanes(p_ref, here, lambda c: jnp.exp2(s_s[here, c] * factor - top).astype(bf16))
        return carry

    small = rows * s_s.shape[1] <= 2**19
    lax.fori_loop(0, rows // CHUNK, step, 0, unroll=rows // CHUNK if small else 7)


def blocks(total, rows, columns):
    size = total if total * columns <= 2**19 else rows
    return [slice(a, a + size) for a in range(0, total, size)]


def row_top(s):
    factor = HEAD_DIM ** (-0.5) * LOG2E
    top = jnp.max(s, axis=1, keepdims=True) * factor
    return jnp.broadcast_to(top, (s.shape[0], HEAD_DIM))


def score_grads(ds_s, p, dp, delta):
    for j in range(ds_s.shape[-1] // HEAD_DIM):
        columns = slice(j * HEAD_DIM, (j + 1) * HEAD_DIM)
        ds_s[:, columns] = (p[:, columns].astype(f32) * (dp[:, columns] - delta)).astype(bf16)


def interleave(rows, batch):
    size = rows * batch
    at = lax.broadcasted_iota(jnp.int32, (size, size), 0)
    source = lax.broadcasted_iota(jnp.int32, (size, size), 1)
    return jnp.where(source == (at % rows) * batch + at // rows, 1.0, 0.0).astype(bf16)


def gather_rows(raw_ref, out):
    _, rows, batch, width = raw_ref.shape
    select = interleave(rows, batch)
    group = width // HEAD_DIM
    for g in range(group):
        x = raw_ref[0, :, :, g * HEAD_DIM : (g + 1) * HEAD_DIM].reshape(rows * batch, HEAD_DIM)
        x = mm(select, x).astype(bf16)
        for b in range(batch):
            at = (b * group + g) * rows
            out[at : at + rows, :] = x[b * rows : (b + 1) * rows]


def scatter_rows(view, raw_ref):
    _, rows, batch, width = raw_ref.shape
    select = interleave(rows, batch)
    group = width // HEAD_DIM
    for g in range(group):
        spans = [(b * group + g) * rows for b in range(batch)]
        x = jnp.concatenate([view[at : at + rows, :] for at in spans], axis=0)
        x = mm_tn(select, x).astype(bf16)
        raw_ref[0, :, :, g * HEAD_DIM : (g + 1) * HEAD_DIM] = x.reshape(rows, batch, HEAD_DIM)


def arrange_body(raw_q_ref, raw_do_ref, q_ref, do_ref):
    gather_rows(raw_q_ref, q_ref.at[0])
    gather_rows(raw_do_ref, do_ref.at[0])


def prefix_forward_body(
    bias_ref, q_ref, pa_ref, pb_ref, pc_ref, pd_ref, p_ref, ol_ref, m_ref, k_s, v_s, s_s
):
    batch = bias_ref.shape[0]
    total = q_ref.shape[1]
    per = total // batch
    place_prefix((pa_ref, pb_ref, pc_ref, pd_ref), k_s, v_s)
    v_s[:, HEAD_DIM:] = jnp.ones((v_s.shape[0], HEAD_DIM), bf16)
    for b in range(batch):
        for part in blocks(per, 64, k_s.shape[0]):
            rows = slice(b * per + part.start, b * per + part.stop)
            s = mm_nt(q_ref[0, rows, :], k_s[...]) + bias_ref[b, 0:1, :]
            s_s[rows, :] = s
            m_ref[0, rows, :] = row_top(s)
    for b in range(batch):
        rows = slice(b * per, (b + 1) * per)
        exponents(p_ref, s_s, lambda here: m_ref[0, here, :], b * per, per)
        ol_ref[0, rows, :] = mm(p_ref[0, rows, :], v_s[...])


def middle_body(
    pieces,
    live_ref,
    bias_ref,
    q_ref,
    do_ref,
    ol_ref,
    m_ref,
    *rest,
):
    answer = rest[:pieces]
    (
        out_ref,
        doa_ref,
        deltaa_ref,
        ds_ref,
        *grads,
        s_s,
        ka_s,
        va_s,
        olb_s,
        mb_s,
        p_s,
        dob_s,
        deltab_s,
    ) = rest[pieces:]
    scale = HEAD_DIM ** (-0.5)
    batch = ka_s.shape[0]
    keys = ka_s.shape[1]
    rows = bias_ref.shape[0]
    total = q_ref.shape[1]
    per = total // batch
    groups = per // rows
    columns = head_columns()
    piece_rows = answer[0].shape[-2]
    place_answer(answer, ka_s, va_s)
    va_s[:, :, HEAD_DIM:] = jnp.ones((batch, keys, HEAD_DIM), bf16)
    for b in range(batch):
        for part in blocks(per, rows, keys):
            base = b * per + part.start
            size = part.stop - part.start
            scores = mm_nt(q_ref[0, base : base + size, :], ka_s[b])
            for g in range(size // rows):
                span = slice(base + g * rows, base + (g + 1) * rows)
                s = scores[g * rows : (g + 1) * rows, :] + bias_ref[...]
                s_s[span, :] = s
                mb_s[span, :] = row_top(s)
    for b in range(batch):
        exponents(p_s, s_s, lambda here: mb_s[here, :], b * per, per)
        olb_s[b * per : (b + 1) * per, :] = mm(p_s[0, b * per : (b + 1) * per, :], va_s[b])

    for b in range(batch):

        def combine(i, carry, b=b):
            here = pl.ds(pl.multiple_of(b * per + i * rows, rows), rows)
            live = live_ref[b]
            ma = m_ref[0, here, :]
            mb = mb_s[here, :]
            top = jnp.maximum(ma, mb)
            ea = jnp.exp2(ma - top)
            eb = jnp.exp2(mb - top)
            inverse = 1.0 / (
                ol_ref[0, here, HEAD_DIM:] * ea + olb_s[here, HEAD_DIM:] * eb
            )
            ea = ea * inverse
            eb = eb * inverse
            attended = (ol_ref[0, here, 0:HEAD_DIM] * ea + olb_s[here, 0:HEAD_DIM] * eb) * live
            out_ref[0, here, :] = attended.astype(bf16)
            douts = do_ref[0, here, :].astype(f32) * live
            da = (douts * ea).astype(bf16)
            db = (douts * eb).astype(bf16)
            doa_ref[0, here, :] = da
            dob_s[here, :] = db
            deltaa_ref[0, here, :] = jnp.broadcast_to(
                jnp.sum(da.astype(f32) * attended, axis=1, keepdims=True), (rows, HEAD_DIM)
            )
            deltab_s[here, :] = jnp.broadcast_to(
                jnp.sum(db.astype(f32) * attended, axis=1, keepdims=True), (rows, HEAD_DIM)
            )
            return carry

        lax.fori_loop(0, groups, combine, 0, unroll=groups)
    for b in range(batch):
        for part in blocks(per, rows, keys):
            span = slice(b * per + part.start, b * per + part.stop)
            dp = mm_nt(dob_s[span, :], va_s[b, :, 0:HEAD_DIM])
            score_grads(ds_ref.at[0, span], p_s[0, span, :], dp, deltab_s[span, :])
    for b in range(batch):
        span = slice(b * per, (b + 1) * per)
        value_term = jnp.transpose(mm_tn(dob_s[span, :], p_s[0, span, :])).astype(bf16)
        key_term = (jnp.transpose(mm_tn(q_ref[0, span, :], ds_ref[0, span, :])) * scale).astype(bf16)
        for t in range(pieces):
            part = slice(t * piece_rows, (t + 1) * piece_rows)
            ref = grads[4 * t // pieces]
            ref[t % (pieces // 4), 0, b, :, columns] = key_term[part]
            ref[t % (pieces // 4), 1, b, :, columns] = value_term[part]


def prefix_backward_body(q_ref, p_ref, doa_ref, deltaa_ref, *rest):
    prefix = rest[:4]
    ds_ref, own_ref, near_ref, far_ref, k_s, v_s = rest[4:]
    scale = HEAD_DIM ** (-0.5)
    total = q_ref.shape[1]
    place_prefix(prefix, k_s, v_s)
    size = total // 2 if total // 2 * k_s.shape[0] <= 2**19 else 64
    for span in blocks(total, size, k_s.shape[0]):
        dp = mm_nt(doa_ref[0, span, :], v_s[...])
        score_grads(ds_ref.at[0, span], p_ref[0, span, :], dp, deltaa_ref[0, span, :])
    columns = head_columns()
    half = own_ref.shape[1]
    quarter = half // 2
    value_term = jnp.transpose(mm_tn(doa_ref[0], p_ref[0])).astype(bf16)
    key_term = (jnp.transpose(mm_tn(q_ref[0], ds_ref[0])) * scale).astype(bf16)
    for t, term in ((0, key_term), (1, value_term)):
        own_ref[t, :, columns] = term[:half]
        near_ref[t, :, columns] = term[half : half + quarter]
        far_ref[t, :, columns] = term[half + quarter :]


def query_backward_body(pieces, out_ref, dsa_ref, dsb_ref, *rest):
    prefix = rest[:4]
    answer = rest[4 : 4 + pieces]
    raw_out_ref, raw_dq_ref, k_s, ka_s, dq_s = rest[4 + pieces :]
    scale = HEAD_DIM ** (-0.5)
    batch = ka_s.shape[0]
    per = dq_s.shape[0] // batch
    place_prefix(prefix, k_s, None)
    place_answer(answer, ka_s, None)
    for b in range(batch):
        rows = slice(b * per, (b + 1) * per)
        dq = mm(dsa_ref[0, rows, :], k_s[...]) + mm(dsb_ref[0, rows, :], ka_s[b])
        dq_s[rows, :] = (dq * scale).astype(bf16)
    scatter_rows(out_ref.at[0], raw_out_ref)
    scatter_rows(dq_s, raw_dq_ref)


def on_device(
    queries,
    answer_keys,
    answer_values,
    prefix_keys,
    prefix_values,
    grad_out,
    answer_length,
    prefix_limit,
):
    size = lax.axis_size("seq")
    sides = lax.axis_size("pair")
    assert sides == 2 and size >= 4 and size & (size - 1) == 0
    outer = size // 2
    rows = queries.shape[1]
    batch = queries.shape[2]
    kv = answer_keys.shape[3] // HEAD_DIM
    group = queries.shape[3] // HEAD_DIM // kv
    per = group * rows
    total = batch * per
    prefix_rows = prefix_keys.shape[0]
    prefix_total = prefix_rows * size * sides
    answer_total = rows * size
    place = lax.axis_index("seq")
    side = lax.axis_index("pair")
    z, y = place // 2, place % 2

    def swap_z(x, k):
        return lax.ppermute(x, "seq", [(i, i ^ (2 * k)) for i in range(size)])

    def swap_y(x):
        return lax.ppermute(x, "seq", [(i, i ^ 1) for i in range(size)])

    def swap_x(x):
        return lax.ppermute(x, "pair", [(0, 1), (1, 0)])

    prefix_own = jnp.stack([prefix_keys, prefix_values])
    answer_own = jnp.stack([a[0].transpose(1, 0, 2) for a in (answer_keys, answer_values)])
    prefix_z = jnp.stack([prefix_own] + [swap_z(prefix_own, k) for k in range(1, outer)])
    prefix_y = swap_y(prefix_z)
    prefix = [prefix_z, prefix_y, swap_x(prefix_z), swap_x(prefix_y)]
    near = [answer_own] + [swap_z(answer_own, k) for k in range(1, outer)]
    far = [swap_y(piece) for piece in near]
    answer = near + far
    pieces = len(answer)

    dz = jnp.arange(outer, dtype=jnp.int32)
    z_from = z ^ dz
    pair_from = (side + jnp.arange(2, dtype=jnp.int32)) % 2
    y_from = (y + jnp.arange(2, dtype=jnp.int32)) % 2
    seq_from = z_from[None, :] * 2 + y_from[:, None]
    shard = pair_from[:, None, None] * size + seq_from[None]
    spots = (
        shard[..., None] * prefix_rows + jnp.arange(prefix_rows, dtype=jnp.int32)
    ).reshape(prefix_total)
    prefix_bias = jnp.where(spots[None, None, :] < prefix_limit[0][:, None, None], 0.0, NEGATIVE)
    prefix_bias = jnp.broadcast_to(prefix_bias, (batch, 8, prefix_total)).astype(f32)
    row_places = place * rows + jnp.arange(rows, dtype=jnp.int32)
    key_places = (
        seq_from[..., None] * rows + jnp.arange(rows, dtype=jnp.int32)
    ).reshape(answer_total)
    answer_bias = jnp.where(key_places[None, :] <= row_places[:, None], 0.0, NEGATIVE).astype(f32)
    live = jnp.where(row_places[None, :] < answer_length[0][:, None], 1.0, 0.0).astype(f32)
    live = jnp.broadcast_to(live[:, :, None], (batch, rows, HEAD_DIM))

    def whole(shape):
        return pl.BlockSpec(shape, lambda c: (0,) * len(shape))

    def by_head(shape, axis=0):
        block = tuple(1 if a == axis else n for a, n in enumerate(shape))
        return pl.BlockSpec(block, lambda c: tuple(c if a == axis else 0 for a in range(len(shape))))

    raw_spec = pl.BlockSpec((1, rows, batch, group * HEAD_DIM), lambda c: (0, 0, 0, c))
    q_shape = (kv, total, HEAD_DIM)
    q_spec = by_head(q_shape)
    prefix_specs = [whole(prefix_z.shape)] * 4
    answer_spec = whole(answer_own.shape)
    pa_shape = (kv, total, prefix_total)
    pb_shape = (kv, total, answer_total)
    ol_shape = (kv, total, 2 * HEAD_DIM)
    own_shape = (2, prefix_total // 2, kv * HEAD_DIM)
    sent_shape = (2, prefix_total // 4, kv * HEAD_DIM)
    stack_shape = (outer // 2,) + answer_own.shape
    unit_a = 2 * kv * total * prefix_total * HEAD_DIM
    unit_b = 2 * kv * total * answer_total * HEAD_DIM

    query_view, grad_view = pl.pallas_call(
        arrange_body,
        grid=(kv,),
        in_specs=[raw_spec, raw_spec],
        out_specs=[q_spec, q_spec],
        out_shape=[jax.ShapeDtypeStruct(q_shape, bf16)] * 2,
        compiler_params=params(total * prefix_total),
        cost_estimate=cost(4 * kv * total * HEAD_DIM * HEAD_DIM, 4 << 20, 0),
        name="arrange",
    )(queries, grad_out)

    probs_a, ol_a, top_a = pl.pallas_call(
        prefix_forward_body,
        grid=(kv,),
        in_specs=[whole(prefix_bias.shape), q_spec] + prefix_specs,
        out_specs=[by_head(pa_shape), by_head(ol_shape), q_spec],
        out_shape=[
            jax.ShapeDtypeStruct(pa_shape, bf16),
            jax.ShapeDtypeStruct(ol_shape, f32),
            jax.ShapeDtypeStruct(q_shape, f32),
        ],
        scratch_shapes=[
            pltpu.VMEM((prefix_total, HEAD_DIM), bf16),
            pltpu.VMEM((prefix_total, 2 * HEAD_DIM), bf16),
            pltpu.VMEM((total, prefix_total), f32),
        ],
        compiler_params=params(total * prefix_total),
        cost_estimate=cost(2 * unit_a, 8 << 20, kv * total * prefix_total),
        name="prefix_forward",
    )(prefix_bias, query_view, *prefix)

    (out_view, grad_a, delta_a, ds_b, near_low, near_high, far_low, far_high) = pl.pallas_call(
        lambda *refs: middle_body(pieces, *refs),
        grid=(kv,),
        in_specs=[
            whole(live.shape),
            whole(answer_bias.shape),
            q_spec,
            q_spec,
            by_head(ol_shape),
            q_spec,
        ]
        + [answer_spec] * pieces,
        out_specs=[q_spec, q_spec, q_spec, by_head(pb_shape)] + [whole(stack_shape)] * 4,
        out_shape=[
            jax.ShapeDtypeStruct(q_shape, bf16),
            jax.ShapeDtypeStruct(q_shape, bf16),
            jax.ShapeDtypeStruct(q_shape, f32),
            jax.ShapeDtypeStruct(pb_shape, bf16),
        ]
        + [jax.ShapeDtypeStruct(stack_shape, bf16)] * 4,
        scratch_shapes=[
            pltpu.VMEM((total, answer_total), f32),
            pltpu.VMEM((batch, answer_total, HEAD_DIM), bf16),
            pltpu.VMEM((batch, answer_total, 2 * HEAD_DIM), bf16),
            pltpu.VMEM((total, 2 * HEAD_DIM), f32),
            pltpu.VMEM((total, HEAD_DIM), f32),
            pltpu.VMEM((1, total, answer_total), bf16),
            pltpu.VMEM((total, HEAD_DIM), bf16),
            pltpu.VMEM((total, HEAD_DIM), f32),
        ],
        compiler_params=params(total * prefix_total),
        cost_estimate=cost(5 * unit_b, 12 << 20, kv * total * answer_total),
        name="middle",
    )(live, answer_bias, query_view, grad_view, ol_a, top_a, *answer)

    ds_a, prefix_own_sum, prefix_near, prefix_far = pl.pallas_call(
        prefix_backward_body,
        grid=(kv,),
        in_specs=[q_spec, by_head(pa_shape), q_spec, q_spec] + prefix_specs,
        out_specs=[
            by_head(pa_shape),
            whole(own_shape),
            whole(sent_shape),
            whole(sent_shape),
        ],
        out_shape=[
            jax.ShapeDtypeStruct(pa_shape, bf16),
            jax.ShapeDtypeStruct(own_shape, bf16),
            jax.ShapeDtypeStruct(sent_shape, bf16),
            jax.ShapeDtypeStruct(sent_shape, bf16),
        ],
        scratch_shapes=[
            pltpu.VMEM((prefix_total, HEAD_DIM), bf16),
            pltpu.VMEM((prefix_total, HEAD_DIM), bf16),
        ],
        compiler_params=params(total * prefix_total),
        cost_estimate=cost(3 * unit_a, 12 << 20, 0),
        name="prefix_backward",
    )(query_view, probs_a, grad_a, delta_a, *prefix)

    attention_out, grad_queries = pl.pallas_call(
        lambda *refs: query_backward_body(pieces, *refs),
        grid=(kv,),
        in_specs=[q_spec, by_head(pa_shape), by_head(pb_shape)]
        + prefix_specs
        + [answer_spec] * pieces,
        out_specs=[raw_spec, raw_spec],
        out_shape=[jax.ShapeDtypeStruct(queries.shape, bf16)] * 2,
        scratch_shapes=[
            pltpu.VMEM((prefix_total, HEAD_DIM), bf16),
            pltpu.VMEM((batch, answer_total, HEAD_DIM), bf16),
            pltpu.VMEM((total, HEAD_DIM), bf16),
        ],
        compiler_params=params(total * prefix_total),
        cost_estimate=cost(unit_a + unit_b, 8 << 20, 0),
        name="query_backward",
    )(out_view, ds_a, ds_b, *prefix, *answer)

    split = (2, outer, prefix_rows, kv * HEAD_DIM)
    half = prefix_total // 4
    far_got = swap_x(prefix_far).astype(f32) + prefix_own_sum[:, half:].astype(f32)
    y_got = swap_y(far_got.astype(bf16)).astype(f32)
    near_got = swap_x(prefix_near).astype(f32)
    z_sum = (near_got + prefix_own_sum[:, :half].astype(f32) + y_got).reshape(split)
    prefix_sum = z_sum[:, 0]
    for k in range(1, outer):
        prefix_sum = prefix_sum + swap_z(z_sum[:, k].astype(bf16), k).astype(f32)
    high_got = swap_y(far_high)
    low_got = swap_y(far_low)
    high = (near_high.astype(f32) + high_got.astype(f32)).astype(bf16)
    low = near_low.astype(f32) + low_got.astype(f32)
    answer_sum = low[0]
    for k in range(1, outer):
        at = k % (outer // 2)
        piece = (high if k >= outer // 2 else low)[at]
        answer_sum = answer_sum + swap_z(piece.astype(bf16), k).astype(f32)
    answer_sum = answer_sum.astype(bf16)

    def answer_out(x):
        return x.transpose(1, 0, 2).reshape(answer_keys.shape)

    return (
        attention_out,
        grad_queries,
        answer_out(answer_sum[0]),
        answer_out(answer_sum[1]),
        prefix_sum[0],
        prefix_sum[1],
    )


def solution(mesh):
    wide = P("pair", "seq", None, "head")
    shared = P(("pair", "seq"), "head")
    small = P("pair", None)

    return jax.shard_map(
        on_device,
        mesh=mesh,
        in_specs=(wide, wide, wide, shared, shared, wide, small, small),
        out_specs=(wide, wide, wide, wide, shared, shared),
        check_vma=False,
    )
```

```python
import math

import jax
import jax.numpy as jnp
from jax import lax
from jax.experimental import pallas as pl
from jax.experimental.pallas import tpu as pltpu
from jax.sharding import PartitionSpec as P


HEAD_DIM = 128
NEGATIVE = -1e30
LOG2E = math.log2(math.e)

f32 = jnp.float32
bf16 = jnp.bfloat16
CHUNK = 32


def mm(a, b):
    return jnp.dot(a, b, preferred_element_type=f32)


def mm_nt(a, b):
    return lax.dot_general(a, b, (((1,), (1,)), ((), ())), preferred_element_type=f32)


def mm_tn(a, b):
    return lax.dot_general(a, b, (((0,), (0,)), ((), ())), preferred_element_type=f32)


def params(cells):
    limit = 18 if cells <= 2**20 else 60
    return pltpu.CompilerParams(
        dimension_semantics=("arbitrary",), vmem_limit_bytes=limit * 1024 * 1024
    )


def cost(flops, moved, exps):
    return pl.CostEstimate(flops=flops, bytes_accessed=moved, transcendentals=exps)


def head_columns():
    return pl.ds(pl.multiple_of(pl.program_id(0) * HEAD_DIM, HEAD_DIM), HEAD_DIM)


def place_prefix(refs, k_s, v_s):
    columns = head_columns()
    rows = refs[0].shape[-2]
    at = 0
    for ref in refs:
        for dz in range(ref.shape[0]):
            k_s[at : at + rows, :] = ref[dz, 0, :, columns]
            if v_s is not None:
                v_s[at : at + rows, 0:HEAD_DIM] = ref[dz, 1, :, columns]
            at += rows


def place_answer(refs, k_s, v_s):
    columns = head_columns()
    rows = refs[0].shape[-2]
    for t, ref in enumerate(refs):
        for b in range(ref.shape[1]):
            k_s[b, t * rows : (t + 1) * rows, :] = ref[0, b, :, columns]
            if v_s is not None:
                v_s[b, t * rows : (t + 1) * rows, 0:HEAD_DIM] = ref[1, b, :, columns]


def lanes(ref, here, update):
    for j in range(ref.shape[-1] // HEAD_DIM):
        columns = slice(j * HEAD_DIM, (j + 1) * HEAD_DIM)
        ref[0, here, columns] = update(columns)


def exponents(p_ref, s_s, m_s, first, rows):
    factor = HEAD_DIM ** (-0.5) * LOG2E

    def step(i, carry):
        here = pl.ds(pl.multiple_of(first + i * CHUNK, CHUNK), CHUNK)
        top = m_s(here)
        lanes(p_ref, here, lambda c: jnp.exp2(s_s[here, c] * factor - top).astype(bf16))
        return carry

    small = rows * s_s.shape[1] <= 2**19
    lax.fori_loop(0, rows // CHUNK, step, 0, unroll=rows // CHUNK if small else 7)


def blocks(total, rows, columns):
    size = total if total * columns <= 2**19 else rows
    return [slice(a, a + size) for a in range(0, total, size)]


def row_top(s):
    factor = HEAD_DIM ** (-0.5) * LOG2E
    top = jnp.max(s, axis=1, keepdims=True) * factor
    return jnp.broadcast_to(top, (s.shape[0], HEAD_DIM))


def score_grads(ds_s, p, dp, delta):
    for j in range(ds_s.shape[-1] // HEAD_DIM):
        columns = slice(j * HEAD_DIM, (j + 1) * HEAD_DIM)
        ds_s[:, columns] = (p[:, columns].astype(f32) * (dp[:, columns] - delta)).astype(bf16)


def interleave(rows, batch):
    size = rows * batch
    at = lax.broadcasted_iota(jnp.int32, (size, size), 0)
    source = lax.broadcasted_iota(jnp.int32, (size, size), 1)
    return jnp.where(source == (at % rows) * batch + at // rows, 1.0, 0.0).astype(bf16)


def gather_rows(raw_ref, out):
    _, rows, batch, width = raw_ref.shape
    select = interleave(rows, batch)
    group = width // HEAD_DIM
    for g in range(group):
        x = raw_ref[0, :, :, g * HEAD_DIM : (g + 1) * HEAD_DIM].reshape(rows * batch, HEAD_DIM)
        x = mm(select, x).astype(bf16)
        for b in range(batch):
            at = (b * group + g) * rows
            out[at : at + rows, :] = x[b * rows : (b + 1) * rows]


def scatter_rows(view, raw_ref):
    _, rows, batch, width = raw_ref.shape
    select = interleave(rows, batch)
    group = width // HEAD_DIM
    for g in range(group):
        spans = [(b * group + g) * rows for b in range(batch)]
        x = jnp.concatenate([view[at : at + rows, :] for at in spans], axis=0)
        x = mm_tn(select, x).astype(bf16)
        raw_ref[0, :, :, g * HEAD_DIM : (g + 1) * HEAD_DIM] = x.reshape(rows, batch, HEAD_DIM)


def arrange_body(raw_q_ref, raw_do_ref, q_ref, do_ref):
    gather_rows(raw_q_ref, q_ref.at[0])
    gather_rows(raw_do_ref, do_ref.at[0])


def prefix_forward_body(
    bias_ref, q_ref, pa_ref, pb_ref, pc_ref, pd_ref, p_ref, ol_ref, m_ref, k_s, v_s, s_s
):
    batch = bias_ref.shape[0]
    total = q_ref.shape[1]
    per = total // batch
    place_prefix((pa_ref, pb_ref, pc_ref, pd_ref), k_s, v_s)
    v_s[:, HEAD_DIM:] = jnp.ones((v_s.shape[0], HEAD_DIM), bf16)
    for b in range(batch):
        for part in blocks(per, 64, k_s.shape[0]):
            rows = slice(b * per + part.start, b * per + part.stop)
            s = mm_nt(q_ref[0, rows, :], k_s[...]) + bias_ref[b, 0:1, :]
            s_s[rows, :] = s
            m_ref[0, rows, :] = row_top(s)
    for b in range(batch):
        rows = slice(b * per, (b + 1) * per)
        exponents(p_ref, s_s, lambda here: m_ref[0, here, :], b * per, per)
        ol_ref[0, rows, :] = mm(p_ref[0, rows, :], v_s[...])


def middle_body(
    pieces,
    live_ref,
    bias_ref,
    q_ref,
    do_ref,
    ol_ref,
    m_ref,
    *rest,
):
    answer = rest[:pieces]
    (
        out_ref,
        doa_ref,
        deltaa_ref,
        ds_ref,
        *grads,
        s_s,
        ka_s,
        va_s,
        olb_s,
        mb_s,
        p_s,
        dob_s,
        deltab_s,
    ) = rest[pieces:]
    scale = HEAD_DIM ** (-0.5)
    batch = ka_s.shape[0]
    keys = ka_s.shape[1]
    rows = bias_ref.shape[0]
    total = q_ref.shape[1]
    per = total // batch
    groups = per // rows
    columns = head_columns()
    piece_rows = answer[0].shape[-2]
    place_answer(answer, ka_s, va_s)
    va_s[:, :, HEAD_DIM:] = jnp.ones((batch, keys, HEAD_DIM), bf16)
    for b in range(batch):
        for part in blocks(per, rows, keys):
            base = b * per + part.start
            size = part.stop - part.start
            scores = mm_nt(q_ref[0, base : base + size, :], ka_s[b])
            for g in range(size // rows):
                span = slice(base + g * rows, base + (g + 1) * rows)
                s = scores[g * rows : (g + 1) * rows, :] + bias_ref[...]
                s_s[span, :] = s
                mb_s[span, :] = row_top(s)
    for b in range(batch):
        exponents(p_s, s_s, lambda here: mb_s[here, :], b * per, per)
        olb_s[b * per : (b + 1) * per, :] = mm(p_s[0, b * per : (b + 1) * per, :], va_s[b])

    for b in range(batch):

        def combine(i, carry, b=b):
            for h in range(rows // CHUNK):
                here = pl.ds(pl.multiple_of(b * per + i * rows + h * CHUNK, CHUNK), CHUNK)
                live = live_ref[b, h * CHUNK : (h + 1) * CHUNK]
                ma = m_ref[0, here, :]
                mb = mb_s[here, :]
                top = jnp.maximum(ma, mb)
                ea = jnp.exp2(ma - top)
                eb = jnp.exp2(mb - top)
                inverse = 1.0 / (
                    ol_ref[0, here, HEAD_DIM:] * ea + olb_s[here, HEAD_DIM:] * eb
                )
                ea = ea * inverse
                eb = eb * inverse
                attended = (ol_ref[0, here, 0:HEAD_DIM] * ea + olb_s[here, 0:HEAD_DIM] * eb) * live
                out_ref[0, here, :] = attended.astype(bf16)
                douts = do_ref[0, here, :].astype(f32) * live
                da = (douts * ea).astype(bf16)
                db = (douts * eb).astype(bf16)
                doa_ref[0, here, :] = da
                dob_s[here, :] = db
                deltaa_ref[0, here, :] = jnp.broadcast_to(
                    jnp.sum(da.astype(f32) * attended, axis=1, keepdims=True), (CHUNK, HEAD_DIM)
                )
                deltab_s[here, :] = jnp.broadcast_to(
                    jnp.sum(db.astype(f32) * attended, axis=1, keepdims=True), (CHUNK, HEAD_DIM)
                )
            return carry

        lax.fori_loop(0, groups, combine, 0, unroll=groups)

    def store(t, b, term):
        for piece in range(pieces):
            part = slice(piece * piece_rows, (piece + 1) * piece_rows)
            grads[4 * piece // pieces][piece % (pieces // 4), t, b, :, columns] = term[part]

    for b in range(batch):
        span = slice(b * per, (b + 1) * per)
        store(1, b, jnp.transpose(mm_tn(dob_s[span, :], p_s[0, span, :])).astype(bf16))
        for part in blocks(per, rows, keys):
            some = slice(b * per + part.start, b * per + part.stop)
            dp = mm_nt(dob_s[some, :], va_s[b, :, 0:HEAD_DIM])
            score_grads(ds_ref.at[0, some], p_s[0, some, :], dp, deltab_s[some, :])
    for b in range(batch):
        span = slice(b * per, (b + 1) * per)
        term = jnp.transpose(mm_tn(q_ref[0, span, :], ds_ref[0, span, :])) * scale
        store(0, b, term.astype(bf16))


def prefix_backward_body(q_ref, p_ref, doa_ref, deltaa_ref, *rest):
    prefix = rest[:4]
    ds_ref, own_ref, near_ref, far_ref, k_s, v_s = rest[4:]
    scale = HEAD_DIM ** (-0.5)
    total = q_ref.shape[1]
    place_prefix(prefix, k_s, v_s)
    size = total // 2 if total // 2 * k_s.shape[0] <= 2**19 else 64
    for span in blocks(total, size, k_s.shape[0]):
        dp = mm_nt(doa_ref[0, span, :], v_s[...])
        score_grads(ds_ref.at[0, span], p_ref[0, span, :], dp, deltaa_ref[0, span, :])
    columns = head_columns()
    half = own_ref.shape[1]
    quarter = half // 2
    value_term = jnp.transpose(mm_tn(doa_ref[0], p_ref[0])).astype(bf16)
    key_term = (jnp.transpose(mm_tn(q_ref[0], ds_ref[0])) * scale).astype(bf16)
    for t, term in ((0, key_term), (1, value_term)):
        own_ref[t, :, columns] = term[:half]
        near_ref[t, :, columns] = term[half : half + quarter]
        far_ref[t, :, columns] = term[half + quarter :]


def query_backward_body(pieces, out_ref, dsa_ref, dsb_ref, *rest):
    prefix = rest[:4]
    answer = rest[4 : 4 + pieces]
    raw_out_ref, raw_dq_ref, k_s, ka_s, dq_s = rest[4 + pieces :]
    scale = HEAD_DIM ** (-0.5)
    batch = ka_s.shape[0]
    per = dq_s.shape[0] // batch
    place_prefix(prefix, k_s, None)
    place_answer(answer, ka_s, None)
    for b in range(batch):
        rows = slice(b * per, (b + 1) * per)
        dq = mm(dsa_ref[0, rows, :], k_s[...]) + mm(dsb_ref[0, rows, :], ka_s[b])
        dq_s[rows, :] = (dq * scale).astype(bf16)
    scatter_rows(out_ref.at[0], raw_out_ref)
    scatter_rows(dq_s, raw_dq_ref)


def on_device(
    queries,
    answer_keys,
    answer_values,
    prefix_keys,
    prefix_values,
    grad_out,
    answer_length,
    prefix_limit,
):
    size = lax.axis_size("seq")
    sides = lax.axis_size("pair")
    assert sides == 2 and size >= 4 and size & (size - 1) == 0
    outer = size // 2
    rows = queries.shape[1]
    batch = queries.shape[2]
    kv = answer_keys.shape[3] // HEAD_DIM
    group = queries.shape[3] // HEAD_DIM // kv
    per = group * rows
    total = batch * per
    prefix_rows = prefix_keys.shape[0]
    prefix_total = prefix_rows * size * sides
    answer_total = rows * size
    place = lax.axis_index("seq")
    side = lax.axis_index("pair")
    z, y = place // 2, place % 2

    def swap_z(x, k):
        return lax.ppermute(x, "seq", [(i, i ^ (2 * k)) for i in range(size)])

    def swap_y(x):
        return lax.ppermute(x, "seq", [(i, i ^ 1) for i in range(size)])

    def swap_x(x):
        return lax.ppermute(x, "pair", [(0, 1), (1, 0)])

    prefix_own = jnp.stack([prefix_keys, prefix_values])
    answer_own = jnp.stack([a[0].transpose(1, 0, 2) for a in (answer_keys, answer_values)])
    prefix_z = jnp.stack([prefix_own] + [swap_z(prefix_own, k) for k in range(1, outer)])
    prefix_y = swap_y(prefix_z)
    prefix = [prefix_z, prefix_y, swap_x(prefix_z), swap_x(prefix_y)]
    near = [answer_own] + [swap_z(answer_own, k) for k in range(1, outer)]
    far = [swap_y(piece) for piece in near]
    answer = near + far
    pieces = len(answer)

    dz = jnp.arange(outer, dtype=jnp.int32)
    z_from = z ^ dz
    pair_from = (side + jnp.arange(2, dtype=jnp.int32)) % 2
    y_from = (y + jnp.arange(2, dtype=jnp.int32)) % 2
    seq_from = z_from[None, :] * 2 + y_from[:, None]
    shard = pair_from[:, None, None] * size + seq_from[None]
    spots = (
        shard[..., None] * prefix_rows + jnp.arange(prefix_rows, dtype=jnp.int32)
    ).reshape(prefix_total)
    prefix_bias = jnp.where(spots[None, None, :] < prefix_limit[0][:, None, None], 0.0, NEGATIVE)
    prefix_bias = jnp.broadcast_to(prefix_bias, (batch, 8, prefix_total)).astype(f32)
    row_places = place * rows + jnp.arange(rows, dtype=jnp.int32)
    key_places = (
        seq_from[..., None] * rows + jnp.arange(rows, dtype=jnp.int32)
    ).reshape(answer_total)
    answer_bias = jnp.where(key_places[None, :] <= row_places[:, None], 0.0, NEGATIVE).astype(f32)
    live = jnp.where(row_places[None, :] < answer_length[0][:, None], 1.0, 0.0).astype(f32)
    live = jnp.broadcast_to(live[:, :, None], (batch, rows, HEAD_DIM))

    def whole(shape):
        return pl.BlockSpec(shape, lambda c: (0,) * len(shape))

    def by_head(shape, axis=0):
        block = tuple(1 if a == axis else n for a, n in enumerate(shape))
        return pl.BlockSpec(block, lambda c: tuple(c if a == axis else 0 for a in range(len(shape))))

    raw_spec = pl.BlockSpec((1, rows, batch, group * HEAD_DIM), lambda c: (0, 0, 0, c))
    q_shape = (kv, total, HEAD_DIM)
    q_spec = by_head(q_shape)
    prefix_specs = [whole(prefix_z.shape)] * 4
    answer_spec = whole(answer_own.shape)
    pa_shape = (kv, total, prefix_total)
    pb_shape = (kv, total, answer_total)
    ol_shape = (kv, total, 2 * HEAD_DIM)
    own_shape = (2, prefix_total // 2, kv * HEAD_DIM)
    sent_shape = (2, prefix_total // 4, kv * HEAD_DIM)
    stack_shape = (outer // 2,) + answer_own.shape
    unit_a = 2 * kv * total * prefix_total * HEAD_DIM
    unit_b = 2 * kv * total * answer_total * HEAD_DIM

    query_view, grad_view = pl.pallas_call(
        arrange_body,
        grid=(kv,),
        in_specs=[raw_spec, raw_spec],
        out_specs=[q_spec, q_spec],
        out_shape=[jax.ShapeDtypeStruct(q_shape, bf16)] * 2,
        compiler_params=params(total * prefix_total),
        cost_estimate=cost(4 * kv * total * HEAD_DIM * HEAD_DIM, 4 << 20, 0),
        name="arrange",
    )(queries, grad_out)

    probs_a, ol_a, top_a = pl.pallas_call(
        prefix_forward_body,
        grid=(kv,),
        in_specs=[whole(prefix_bias.shape), q_spec] + prefix_specs,
        out_specs=[by_head(pa_shape), by_head(ol_shape), q_spec],
        out_shape=[
            jax.ShapeDtypeStruct(pa_shape, bf16),
            jax.ShapeDtypeStruct(ol_shape, f32),
            jax.ShapeDtypeStruct(q_shape, f32),
        ],
        scratch_shapes=[
            pltpu.VMEM((prefix_total, HEAD_DIM), bf16),
            pltpu.VMEM((prefix_total, 2 * HEAD_DIM), bf16),
            pltpu.VMEM((total, prefix_total), f32),
        ],
        compiler_params=params(total * prefix_total),
        cost_estimate=cost(2 * unit_a, 8 << 20, kv * total * prefix_total),
        name="prefix_forward",
    )(prefix_bias, query_view, *prefix)

    (out_view, grad_a, delta_a, ds_b, near_low, near_high, far_low, far_high) = pl.pallas_call(
        lambda *refs: middle_body(pieces, *refs),
        grid=(kv,),
        in_specs=[
            whole(live.shape),
            whole(answer_bias.shape),
            q_spec,
            q_spec,
            by_head(ol_shape),
            q_spec,
        ]
        + [answer_spec] * pieces,
        out_specs=[q_spec, q_spec, q_spec, by_head(pb_shape)] + [whole(stack_shape)] * 4,
        out_shape=[
            jax.ShapeDtypeStruct(q_shape, bf16),
            jax.ShapeDtypeStruct(q_shape, bf16),
            jax.ShapeDtypeStruct(q_shape, f32),
            jax.ShapeDtypeStruct(pb_shape, bf16),
        ]
        + [jax.ShapeDtypeStruct(stack_shape, bf16)] * 4,
        scratch_shapes=[
            pltpu.VMEM((total, answer_total), f32),
            pltpu.VMEM((batch, answer_total, HEAD_DIM), bf16),
            pltpu.VMEM((batch, answer_total, 2 * HEAD_DIM), bf16),
            pltpu.VMEM((total, 2 * HEAD_DIM), f32),
            pltpu.VMEM((total, HEAD_DIM), f32),
            pltpu.VMEM((1, total, answer_total), bf16),
            pltpu.VMEM((total, HEAD_DIM), bf16),
            pltpu.VMEM((total, HEAD_DIM), f32),
        ],
        compiler_params=params(total * prefix_total),
        cost_estimate=cost(5 * unit_b, 12 << 20, kv * total * answer_total),
        name="middle",
    )(live, answer_bias, query_view, grad_view, ol_a, top_a, *answer)

    ds_a, prefix_own_sum, prefix_near, prefix_far = pl.pallas_call(
        prefix_backward_body,
        grid=(kv,),
        in_specs=[q_spec, by_head(pa_shape), q_spec, q_spec] + prefix_specs,
        out_specs=[
            by_head(pa_shape),
            whole(own_shape),
            whole(sent_shape),
            whole(sent_shape),
        ],
        out_shape=[
            jax.ShapeDtypeStruct(pa_shape, bf16),
            jax.ShapeDtypeStruct(own_shape, bf16),
            jax.ShapeDtypeStruct(sent_shape, bf16),
            jax.ShapeDtypeStruct(sent_shape, bf16),
        ],
        scratch_shapes=[
            pltpu.VMEM((prefix_total, HEAD_DIM), bf16),
            pltpu.VMEM((prefix_total, HEAD_DIM), bf16),
        ],
        compiler_params=params(total * prefix_total),
        cost_estimate=cost(3 * unit_a, 12 << 20, 0),
        name="prefix_backward",
    )(query_view, probs_a, grad_a, delta_a, *prefix)

    attention_out, grad_queries = pl.pallas_call(
        lambda *refs: query_backward_body(pieces, *refs),
        grid=(kv,),
        in_specs=[q_spec, by_head(pa_shape), by_head(pb_shape)]
        + prefix_specs
        + [answer_spec] * pieces,
        out_specs=[raw_spec, raw_spec],
        out_shape=[jax.ShapeDtypeStruct(queries.shape, bf16)] * 2,
        scratch_shapes=[
            pltpu.VMEM((prefix_total, HEAD_DIM), bf16),
            pltpu.VMEM((batch, answer_total, HEAD_DIM), bf16),
            pltpu.VMEM((total, HEAD_DIM), bf16),
        ],
        compiler_params=params(total * prefix_total),
        cost_estimate=cost(unit_a + unit_b, 8 << 20, 0),
        name="query_backward",
    )(out_view, ds_a, ds_b, *prefix, *answer)

    split = (2, outer, prefix_rows, kv * HEAD_DIM)
    half = prefix_total // 4
    far_got = swap_x(prefix_far).astype(f32) + prefix_own_sum[:, half:].astype(f32)
    y_got = swap_y(far_got.astype(bf16)).astype(f32)
    near_got = swap_x(prefix_near).astype(f32)
    z_sum = (near_got + prefix_own_sum[:, :half].astype(f32) + y_got).reshape(split)
    prefix_sum = z_sum[:, 0]
    for k in range(1, outer):
        prefix_sum = prefix_sum + swap_z(z_sum[:, k].astype(bf16), k).astype(f32)
    high_got = swap_y(far_high)
    low_got = swap_y(far_low)
    high = (near_high.astype(f32) + high_got.astype(f32)).astype(bf16)
    low = near_low.astype(f32) + low_got.astype(f32)
    answer_sum = low[0]
    for k in range(1, outer):
        at = k % (outer // 2)
        piece = (high if k >= outer // 2 else low)[at]
        answer_sum = answer_sum + swap_z(piece.astype(bf16), k).astype(f32)
    answer_sum = answer_sum.astype(bf16)

    def answer_out(x):
        return x.transpose(1, 0, 2).reshape(answer_keys.shape)

    return (
        attention_out,
        grad_queries,
        answer_out(answer_sum[0]),
        answer_out(answer_sum[1]),
        prefix_sum[0],
        prefix_sum[1],
    )


def solution(mesh):
    wide = P("pair", "seq", None, "head")
    shared = P(("pair", "seq"), "head")
    small = P("pair", None)

    return jax.shard_map(
        on_device,
        mesh=mesh,
        in_specs=(wide, wide, wide, shared, shared, wide, small, small),
        out_specs=(wide, wide, wide, wide, shared, shared),
        check_vma=False,
    )
```
